512 devices in a mesh: dp: 64 (over z, y_lo, core), mp: 8 (over x, y_hi).
Axes of the slice: x: 4, y: 4 (y_hi: 2, y_lo: 2; y = y_hi * 2 + y_lo), z: 16, core: 2. Of those that a mesh axis runs over, the one named last changes fastest.
Arguments:
- picture_tower_vectors: bfloat16 [12288, 1152], P('dp'), may hold values from -6 to 6
- caption_tower_vectors: bfloat16 [12288, 1152], P('dp', 'mp'), may hold values from -6 to 6
- picture_standardize_factor: float32 [1152], replicated, may hold values from 0.1 to 1.9
- picture_entry_matrix: bfloat16 [1152, 4304], P(None, 'mp'), may hold values from -0.1875 to 0.1875
- picture_exit_matrix: bfloat16 [4304, 1152], P('mp'), may hold values from -0.09375 to 0.09375
- caption_mapping_matrix: bfloat16 [1152, 1152], P('mp'), may hold values from -1 to 1
- energy_multiplier: float32 [], replicated, may hold values from 4 to 16
- energy_offset_term: float32 [], replicated, may hold values from -2 to -0.5
Outputs:
- grad_image: float32 [12288, 1152], P('dp', 'mp')
- grad_text: float32 [12288, 1152], P('dp', 'mp')
The draws below stay inside these ranges and needn't reach their ends.
All inputs are finite; a program needn't handle non-finite values.
Results may differ from the reference program's by a relative error of at most 0.0046.
Values may be sent and summed in bfloat16 or wider, within the bound.
No kernel may reach another device: no remote copies, remote signals or barrier semaphores. Data moves between devices by JAX's collectives and lax.ppermute only.
A program may use at most 64 MiB of HBM per device.

```python
import math
import jax
import jax.numpy as jnp
from jax import lax

D = 1152
FF = 4304
ROWS = 192
PAIRS = 12288
N_DP = 64


def cluster_centres(key):
    anchor_rows = jax.random.normal(jax.random.fold_in(key, 101), (8, D), jnp.float32)
    prototypes = jnp.concatenate([anchor_rows, -anchor_rows], axis=0)
    labels = jax.random.randint(jax.random.fold_in(key, 102), (PAIRS,), 0, 16)
    return prototypes[labels]


def mapping_weights(key):
    entries = jax.random.normal(jax.random.fold_in(key, 103), (D, D), jnp.float32)
    return jnp.clip(entries * (1.0 / math.sqrt(D)), -1.0, 1.0)


def jitter_rows(key):
    return jax.random.normal(key, (PAIRS, D), jnp.float32)


def mix_weights():
    return (0.8, 0.6)


def draw_picture_tower_vectors(key, part):
    centres = cluster_centres(key)
    cluster_weight, jitter_weight = mix_weights()
    values = cluster_weight * centres + jitter_weight * jitter_rows(jax.random.fold_in(key, 104))
    return jnp.clip(values, -6.0, 6.0).astype(jnp.bfloat16)


def draw_caption_tower_vectors(key, part):
    centres = cluster_centres(key)
    mapped = lax.dot_general(centres, mapping_weights(key), (((1,), (1,)), ((), ())), precision=lax.Precision.HIGHEST)
    cluster_weight, jitter_weight = mix_weights()
    values = cluster_weight * mapped + jitter_weight * jitter_rows(jax.random.fold_in(key, 105))
    return jnp.clip(values, -6.0, 6.0).astype(jnp.bfloat16)


def draw_caption_mapping_matrix(key, part):
    return mapping_weights(key).astype(jnp.bfloat16)


def shard_levels(rng, dims, cuts, low, largest):
    level = 1.0
    for axis_at, shards_of in cuts:
        steps = jax.random.uniform(jax.random.fold_in(jax.random.fold_in(rng, 6), axis_at), (shards_of,), jnp.float32, low / len(cuts), largest / len(cuts))
        level = level * jnp.repeat(jnp.exp(steps), dims[axis_at] // shards_of).reshape((-1,) + (1,) * (len(dims) - 1 - axis_at))
    return level


def gaussian(own_key, extent, scale, most, pieces=(), kind=jnp.bfloat16):
    level = shard_levels(own_key, extent, pieces, -0.22, 0.18) if pieces else 1.0
    result = jax.random.normal(own_key, extent, jnp.float32) * scale * level
    return jnp.minimum(jnp.maximum(result, -most), most).astype(kind)


def setup_inputs(seed: int = 0) -> dict:
    arg_keys = jax.random.split(jax.random.key(seed), 9)
    return {
        "picture_tower_vectors": draw_picture_tower_vectors(jax.random.fold_in(arg_keys[8], 71), 0),
        "caption_tower_vectors": draw_caption_tower_vectors(jax.random.fold_in(arg_keys[8], 71), 0),
        "picture_standardize_factor": jnp.clip(1.0 + 0.18 * jax.random.normal(arg_keys[2], (D,), jnp.float32), 0.1, 1.9),
        "picture_entry_matrix": gaussian(arg_keys[3], (D, FF), D ** -0.5, 0.1875, ((1, 8),)),
        "picture_exit_matrix": gaussian(arg_keys[4], (FF, D), FF ** -0.5, 0.09375, ((0, 8),)),
        "caption_mapping_matrix": draw_caption_mapping_matrix(jax.random.fold_in(arg_keys[8], 71), 0),
        "energy_multiplier": jnp.clip(jnp.exp(jax.random.uniform(arg_keys[6], (), jnp.float32, math.log(4.0), math.log(16.0))), 4.0, 16.0),
        "energy_offset_term": jnp.clip(jax.random.uniform(arg_keys[7], (), jnp.float32, -2.0, -0.5), -2.0, -0.5),
    }


def gelu_tanh(values):
    return jax.nn.gelu(values, approximate=True)

def norm_back(upstream, unit_rows, inverse):
    unit_float = unit_rows.astype(jnp.float32)
    along = lax.optimization_barrier(jnp.sum(unit_float * upstream, axis=-1, keepdims=True))
    return inverse * (upstream - unit_float * along)

def reference(picture_tower_vectors, caption_tower_vectors, picture_standardize_factor, picture_entry_matrix, picture_exit_matrix, caption_mapping_matrix, energy_multiplier, energy_offset_term):
    image_float = picture_tower_vectors.astype(jnp.float32)
    mean_row = lax.optimization_barrier(jnp.mean(image_float, axis=-1, keepdims=True))
    variance = lax.optimization_barrier(jnp.mean((image_float - mean_row) ** 2, axis=-1, keepdims=True))
    inv_std = lax.rsqrt(variance + 1e-06)
    centred = (image_float - mean_row) * inv_std
    normed = (centred * picture_standardize_factor).astype(jnp.bfloat16)
    preact = jnp.dot(normed, picture_entry_matrix, preferred_element_type=jnp.float32)
    hidden = gelu_tanh(preact).astype(jnp.bfloat16)
    image_out = image_float + jnp.dot(hidden, picture_exit_matrix, preferred_element_type=jnp.float32)
    inv_image = lax.rsqrt(lax.optimization_barrier(jnp.sum(image_out * image_out, axis=-1, keepdims=True)) + 1e-06)
    unit_image = (image_out * inv_image).astype(jnp.bfloat16)
    text_out = jnp.dot(caption_tower_vectors, caption_mapping_matrix, preferred_element_type=jnp.float32)
    inv_text = lax.rsqrt(lax.optimization_barrier(jnp.sum(text_out * text_out, axis=-1, keepdims=True)) + 1e-06)
    unit_text = (text_out * inv_text).astype(jnp.bfloat16)
    total = ROWS * N_DP
    image_ids = jnp.arange(total, dtype=jnp.int32)

    def block_step(image_dir, block_index):
        first = (block_index * ROWS).astype(jnp.int32)
        block_now = lax.dynamic_slice_in_dim(unit_text, first, ROWS, 0)
        text_ids = first + jnp.arange(ROWS, dtype=jnp.int32)
        cosine_matrix = lax.dot_general(block_now, unit_image, (((1,), (1,)), ((), ())), preferred_element_type=jnp.float32)
        couple_energies = energy_multiplier * cosine_matrix + energy_offset_term
        match_polarity = jnp.where(text_ids[:, None] == image_ids[None, :], 1.0, -1.0).astype(jnp.float32)
        polarity_scaled_energies = (energy_multiplier * -match_polarity * jax.nn.sigmoid(-match_polarity * couple_energies)).astype(jnp.bfloat16)
        image_dir = image_dir + lax.dot_general(polarity_scaled_energies, block_now, (((0,), (0,)), ((), ())), preferred_element_type=jnp.float32)
        text_part = jnp.dot(polarity_scaled_energies, unit_image, preferred_element_type=jnp.float32)
        return (image_dir, text_part)
    image_dir, text_parts = lax.scan(block_step, jnp.zeros((total, D), jnp.float32), jnp.arange(N_DP, dtype=jnp.int32))
    text_dir = text_parts.reshape(total, D)
    grad_out = norm_back(image_dir, unit_image, inv_image)
    grad_out_b = grad_out.astype(jnp.bfloat16)
    grad_hidden = lax.dot_general(grad_out_b, picture_exit_matrix, (((1,), (1,)), ((), ())), preferred_element_type=jnp.float32)
    unused, pull_back = jax.vjp(gelu_tanh, preact)
    grad_pre = pull_back(grad_hidden)[0].astype(jnp.bfloat16)
    grad_normed = lax.dot_general(grad_pre, picture_entry_matrix, (((1,), (1,)), ((), ())), preferred_element_type=jnp.float32)
    scaled = grad_normed * picture_standardize_factor
    mean_one = lax.optimization_barrier(jnp.mean(scaled, axis=-1, keepdims=True))
    mean_two = lax.optimization_barrier(jnp.mean(scaled * centred, axis=-1, keepdims=True))
    grad_image = grad_out + inv_std * (scaled - mean_one - centred * mean_two)
    grad_text_out = norm_back(text_dir, unit_text, inv_text).astype(jnp.bfloat16)
    grad_text = lax.dot_general(grad_text_out, caption_mapping_matrix, (((1,), (1,)), ((), ())), preferred_element_type=jnp.float32)
    return (grad_image, grad_text)
```

```python
import jax
import jax.numpy as jnp
from jax import lax
from jax.sharding import Mesh
from jax.sharding import PartitionSpec as P

DP = ("zh", "zl", "yl", "c")
MP = ("x", "yh")
YY = ("yl", "yh")
F32 = jnp.float32
BF16 = jnp.bfloat16


def swap(array, axes):
    return lax.all_to_all(array, axes, 0, 0, tiled=True)


def exchange(array, axes, k):
    n = lax.axis_size(axes)
    return lax.ppermute(array, axes, [(i, i ^ k) for i in range(n)])


def spread(array, axes):
    n = lax.axis_size(axes)
    copies = jnp.broadcast_to(array[None], (n, *array.shape))
    return swap(copies, axes).reshape(n * array.shape[0], *array.shape[1:])


def summed_at(array, axes):
    n = lax.axis_size(axes)
    parts = array.reshape(n, array.shape[0] // n, *array.shape[1:])
    return jnp.sum(swap(parts, axes).astype(F32), axis=0)


def ring_gather(array, axes):
    n = lax.axis_size(axes)
    parts = [array] + [exchange(array, axes, k) for k in range(1, n)]
    return jnp.concatenate(parts, axis=0)


def ring_sum(array, axes):
    n = lax.axis_size(axes)
    rows = array.shape[0] // n
    total = array[:rows].astype(F32)
    for k in range(1, n):
        piece = array[k * rows : (k + 1) * rows].astype(BF16)
        total = total + exchange(piece, axes, k).astype(F32)
    return total


def gelu_tanh(values):
    return jax.nn.gelu(values, approximate=True)


def norm_back(upstream, unit_rows, inverse):
    unit_float = unit_rows.astype(F32)
    along = jnp.sum(unit_float * upstream, axis=-1, keepdims=True)
    return inverse * (upstream - unit_float * along)


def dot(a, b, dims):
    return lax.dot_general(a, b, (dims, ((), ())), preferred_element_type=F32)


def per_device(picture, caption, gain, entry, exit_matrix, mapping, scale, offset):
    rows = picture.shape[0]
    width = picture.shape[1]
    heads = lax.axis_size(MP)
    head_pos = lax.axis_index(MP)
    share = rows // heads
    cols = caption.shape[1]
    first_row = head_pos * share
    first_col = head_pos * cols
    text_part = dot(caption, mapping, ((1,), (0,))).astype(BF16)
    text_out = summed_at(text_part, MP)
    inv_text = lax.rsqrt(jnp.sum(text_out * text_out, axis=-1, keepdims=True) + 1e-06)
    unit_text = (text_out * inv_text).astype(BF16)

    image_float = picture.astype(F32)
    mean_row = jnp.mean(image_float, axis=-1, keepdims=True)
    variance = jnp.mean((image_float - mean_row) ** 2, axis=-1, keepdims=True)
    inv_std = lax.rsqrt(variance + 1e-06)
    centred = (image_float - mean_row) * inv_std
    normed = (centred * gain).astype(BF16)
    preact = dot(normed, entry, ((1,), (0,)))
    hidden = gelu_tanh(preact).astype(BF16)
    partial_out = dot(hidden, exit_matrix, ((1,), (0,))).astype(BF16)
    own_rows = lax.dynamic_slice_in_dim(picture, first_row, share, 0).astype(F32)
    image_out = own_rows + summed_at(partial_out, MP)
    inv_image = lax.rsqrt(jnp.sum(image_out * image_out, axis=-1, keepdims=True) + 1e-06)
    unit_image = (image_out * inv_image).astype(BF16)

    texts = ring_gather(ring_gather(ring_gather(unit_text, "zh"), YY), "c")
    images = spread(spread(unit_image, "zl"), "x")

    own_start = (lax.axis_index("x") * lax.axis_size("zl") + lax.axis_index("zl")) * share
    text_ids = jnp.arange(texts.shape[0], dtype=jnp.int32)[:, None]
    image_ids = jnp.arange(images.shape[0], dtype=jnp.int32)[None, :] - own_start
    same = (text_ids == image_ids) & (text_ids < share)
    energies = scale * dot(texts, images, ((1,), (1,))) + offset
    polarity = jnp.where(same, 1.0, -1.0).astype(F32)
    weighted = (scale * -polarity * jax.nn.sigmoid(-polarity * energies)).astype(BF16)
    image_add = dot(weighted, texts, ((0,), (0,)))
    text_add = dot(weighted, images, ((1,), (0,)))

    image_half = summed_at(image_add.astype(BF16), "x")
    image_dir = summed_at(image_half.astype(BF16), "zl")
    grad_share = norm_back(image_dir, unit_image, inv_image).astype(BF16)
    grad_out_b = spread(grad_share, MP)

    text_dir = ring_sum(ring_sum(ring_sum(text_add, "c"), YY), "zh")
    grad_text_share = norm_back(text_dir, unit_text, inv_text).astype(BF16)

    grad_hidden = dot(grad_out_b, exit_matrix, ((1,), (1,)))
    unused, pull_back = jax.vjp(gelu_tanh, preact)
    grad_pre = pull_back(grad_hidden)[0].astype(BF16)
    partial_normed = dot(grad_pre, entry, ((1,), (1,)))
    scaled_part = partial_normed * gain
    sums = jnp.stack(
        [jnp.sum(scaled_part, axis=-1), jnp.sum(scaled_part * centred, axis=-1)], axis=-1
    )
    sums_high = lax.reduce_precision(sums, 8, 7)
    sums_low = sums - sums_high
    sums_both = jnp.concatenate([sums_high, sums_low], axis=-1).astype(BF16)
    blocks = partial_normed.astype(BF16).reshape(rows, heads, cols).transpose(1, 0, 2)
    packed = jnp.concatenate(
        [blocks, jnp.broadcast_to(sums_both[None], (heads, *sums_both.shape))], axis=2
    )
    arrived = jnp.sum(swap(packed, MP).astype(F32), axis=0)
    means = (arrived[:, cols : cols + 2] + arrived[:, cols + 2 :]) / width
    gain_here = lax.dynamic_slice_in_dim(gain, first_col, cols, 0)
    feature = jnp.arange(width, dtype=jnp.int32)[:, None] - first_col
    chosen = (feature == jnp.arange(cols, dtype=jnp.int32)[None, :]).astype(BF16)
    picture_here = dot(picture, chosen, ((1,), (0,)))
    centred_here = (picture_here - mean_row) * inv_std
    grad_out_here = dot(grad_out_b, chosen, ((1,), (0,)))
    scaled = arrived[:, :cols] * gain_here
    grad_image = grad_out_here + inv_std * (
        scaled - means[:, :1] - centred_here * means[:, 1:]
    )
    grad_text = dot(spread(grad_text_share, MP), mapping, ((1,), (1,)))
    return (grad_image, grad_text)


def solution(mesh):
    split = Mesh(mesh.devices.reshape(4, 4, 2, 2, 4, 2), (*DP, *MP))
    in_specs = (
        P(DP, None),
        P(DP, MP),
        P(),
        P(None, MP),
        P(MP, None),
        P(MP, None),
        P(),
        P(),
    )
    out_specs = (P(DP, MP), P(DP, MP))
    return jax.shard_map(
        per_device, mesh=split, in_specs=in_specs, out_specs=out_specs, check_vma=False
    )
```

```python
import jax
import jax.numpy as jnp
from jax import lax
from jax.sharding import Mesh
from jax.sharding import PartitionSpec as P


DP = ("zh", "zl", "yl", "c")
MP = ("x", "yh")
Z = ("zh", "zl")
XY = ("yl", "x", "yh")
NEAR = (-2, -1, 1, 2)
FAR = 5
F32 = jnp.float32
BF16 = jnp.bfloat16


def swap(array, axes):
    return lax.all_to_all(array, axes, 0, 0, tiled=True)


def exchange(array, axes, k):
    n = lax.axis_size(axes)
    return lax.ppermute(array, axes, [(i, i ^ k) for i in range(n)])


def spread(array, axes):
    n = lax.axis_size(axes)
    copies = jnp.broadcast_to(array[None], (n, *array.shape))
    return swap(copies, axes).reshape(n * array.shape[0], *array.shape[1:])


def summed_at(array, axes):
    n = lax.axis_size(axes)
    parts = array.reshape(n, array.shape[0] // n, *array.shape[1:])
    return jnp.sum(swap(parts, axes).astype(F32), axis=0)


def shift(array, axes, k):
    n = lax.axis_size(axes)
    return lax.ppermute(array, axes, [(i, (i + k) % n) for i in range(n)])


def gather(array, axes):
    return lax.all_gather(array, axes, axis=0, tiled=True)


def gathered_from_own(array):
    high, low = (lax.axis_size(a) for a in Z)
    rows = array.shape[0]
    spaced = gather(array, "zh")
    parts = gather(spaced, "zl").reshape(low, high, rows, -1)
    in_line = parts.transpose(1, 0, 2, 3).reshape(high * low * rows, -1)
    twice = jnp.concatenate([in_line, in_line], axis=0)
    return lax.dynamic_slice_in_dim(twice, lax.axis_index(Z) * rows, in_line.shape[0], 0)


def sum_over_line(array, share):
    n = lax.axis_size(Z)
    half = n // 2

    def block(k):
        first = (k % n) * share
        return array[first : first + share]

    own = [block(0), block(FAR), block(-FAR)]
    arrived = []
    for b in NEAR:
        parts = [block(b), block(b + FAR), block(b - FAR)]
        arrived.append(shift(jnp.concatenate(parts, axis=0).astype(BF16), Z, b))
    last = shift(block(half).astype(BF16), Z, half - FAR).astype(F32)
    sums = []
    for place in range(3):
        total = own[place]
        for piece in arrived:
            total = total + piece[place * share : (place + 1) * share].astype(F32)
        sums.append(total)
    up = shift((sums[1] + last).astype(BF16), Z, FAR)
    down = shift(sums[2].astype(BF16), Z, -FAR)
    return sums[0] + up.astype(F32) + down.astype(F32)


def gelu_tanh(values):
    return jax.nn.gelu(values, approximate=True)


def norm_back(upstream, unit_rows, inverse):
    unit_float = unit_rows.astype(F32)
    along = jnp.sum(unit_float * upstream, axis=-1, keepdims=True)
    return inverse * (upstream - unit_float * along)


def dot(a, b, dims):
    return lax.dot_general(a, b, (dims, ((), ())), preferred_element_type=F32)


def per_device(picture, caption, gain, entry, exit_matrix, mapping, scale, offset):
    rows = picture.shape[0]
    width = picture.shape[1]
    heads = lax.axis_size(MP)
    head_pos = lax.axis_index(MP)
    share = rows // heads
    cols = caption.shape[1]
    first_row = head_pos * share
    first_col = head_pos * cols
    text_part = dot(caption, mapping, ((1,), (0,))).astype(BF16)
    text_out = summed_at(text_part, MP)
    inv_text = lax.rsqrt(jnp.sum(text_out * text_out, axis=-1, keepdims=True) + 1e-06)
    unit_text = (text_out * inv_text).astype(BF16)

    image_float = picture.astype(F32)
    mean_row = jnp.mean(image_float, axis=-1, keepdims=True)
    variance = jnp.mean((image_float - mean_row) ** 2, axis=-1, keepdims=True)
    inv_std = lax.rsqrt(variance + 1e-06)
    centred = (image_float - mean_row) * inv_std
    normed = (centred * gain).astype(BF16)
    preact = dot(normed, entry, ((1,), (0,)))
    hidden = gelu_tanh(preact).astype(BF16)
    partial_out = dot(hidden, exit_matrix, ((1,), (0,))).astype(BF16)
    own_rows = lax.dynamic_slice_in_dim(picture, first_row, share, 0).astype(F32)
    image_out = own_rows + summed_at(partial_out, MP)
    inv_image = lax.rsqrt(jnp.sum(image_out * image_out, axis=-1, keepdims=True) + 1e-06)
    unit_image = (image_out * inv_image).astype(BF16)

    line = gathered_from_own(unit_text)
    texts = jnp.concatenate([line, exchange(line, "c", 1)], axis=0)
    images = spread(unit_image, XY)

    own_start = lax.axis_index(XY) * share
    text_ids = jnp.arange(texts.shape[0], dtype=jnp.int32)[:, None]
    image_ids = jnp.arange(images.shape[0], dtype=jnp.int32)[None, :] - own_start
    same = (text_ids == image_ids) & (text_ids < share)
    energies = scale * dot(texts, images, ((1,), (1,))) + offset
    polarity = jnp.where(same, 1.0, -1.0).astype(F32)
    weighted = (scale * -polarity * jax.nn.sigmoid(-polarity * energies)).astype(BF16)
    text_add = dot(weighted, images, ((1,), (0,)))
    image_add = dot(weighted, texts, ((0,), (0,)))

    image_parts = swap(image_add.astype(BF16).reshape(-1, share, width), XY)
    image_dir = jnp.sum(image_parts.astype(F32), axis=0)
    grad_share = norm_back(image_dir, unit_image, inv_image).astype(BF16)
    grad_out_b = spread(grad_share, MP)

    middle = text_add.shape[0] // 2
    swapped = exchange(text_add[middle:].astype(BF16), "c", 1)
    text_half = text_add[:middle] + swapped.astype(F32)
    text_dir = sum_over_line(text_half, share)
    grad_text_share = norm_back(text_dir, unit_text, inv_text).astype(BF16)

    grad_hidden = dot(grad_out_b, exit_matrix, ((1,), (1,)))
    _, pull_back = jax.vjp(gelu_tanh, preact)
    grad_pre = pull_back(grad_hidden)[0].astype(BF16)
    partial_normed = dot(grad_pre, entry, ((1,), (1,)))
    scaled_part = partial_normed * gain
    sums = jnp.stack(
        [jnp.sum(scaled_part, axis=-1), jnp.sum(scaled_part * centred, axis=-1)], axis=-1
    )
    sums_high = lax.reduce_precision(sums, 8, 7)
    sums_low = sums - sums_high
    sums_both = jnp.concatenate([sums_high, sums_low], axis=-1).astype(BF16)
    blocks = partial_normed.astype(BF16).reshape(rows, heads, cols).transpose(1, 0, 2)
    packed = jnp.concatenate(
        [blocks, jnp.broadcast_to(sums_both[None], (heads, *sums_both.shape))], axis=2
    )
    arrived = jnp.sum(swap(packed, MP).astype(F32), axis=0)
    means = (arrived[:, cols : cols + 2] + arrived[:, cols + 2 :]) / width
    gain_here = lax.dynamic_slice_in_dim(gain, first_col, cols, 0)
    feature = jnp.arange(width, dtype=jnp.int32)[:, None] - first_col
    chosen = (feature == jnp.arange(cols, dtype=jnp.int32)[None, :]).astype(BF16)
    picture_here = dot(picture, chosen, ((1,), (0,)))
    centred_here = (picture_here - mean_row) * inv_std
    grad_out_here = dot(grad_out_b, chosen, ((1,), (0,)))
    scaled = arrived[:, :cols] * gain_here
    grad_image = grad_out_here + inv_std * (
        scaled - means[:, :1] - centred_here * means[:, 1:]
    )
    grad_text = dot(spread(grad_text_share, MP), mapping, ((1,), (1,)))
    return (grad_image, grad_text)


def solution(mesh):
    split = Mesh(mesh.devices.reshape(4, 4, 2, 2, 4, 2), (*DP, *MP))
    in_specs = (
        P(DP, None),
        P(DP, MP),
        P(),
        P(None, MP),
        P(MP, None),
        P(MP, None),
        P(),
        P(),
    )
    out_specs = (P(DP, MP), P(DP, MP))
    return jax.shard_map(
        per_device, mesh=split, in_specs=in_specs, out_specs=out_specs, check_vma=False
    )
```

```python
import jax
import jax.numpy as jnp
from jax import lax
from jax.sharding import Mesh
from jax.sharding import PartitionSpec as P


DP = ("zh", "zl", "yl", "c")
MP = ("x", "yh")
Z = ("zh", "zl")
XY = ("yl", "x", "yh")
NEAR = (-2, -1, 1, 2)
FAR = 5
F32 = jnp.float32
BF16 = jnp.bfloat16


def swap(array, axes):
    return lax.all_to_all(array, axes, 0, 0, tiled=True)


def exchange(array, axes, k):
    n = lax.axis_size(axes)
    return lax.ppermute(array, axes, [(i, i ^ k) for i in range(n)])


def spread(array, axes):
    n = lax.axis_size(axes)
    copies = jnp.broadcast_to(array[None], (n, *array.shape))
    return swap(copies, axes).reshape(n * array.shape[0], *array.shape[1:])


def shift(array, axes, k):
    n = lax.axis_size(axes)
    return lax.ppermute(array, axes, [(i, (i + k) % n) for i in range(n)])


def gather(array, axes):
    return lax.all_gather(array, axes, axis=0, tiled=True)


def gathered_from_own(array):
    in_line = gather(array, Z)
    twice = jnp.concatenate([in_line, in_line], axis=0)
    first = lax.axis_index(Z) * array.shape[0]
    return lax.dynamic_slice_in_dim(twice, first, in_line.shape[0], 0)


def sum_over_line(array, share):
    n = lax.axis_size(Z)
    half = n // 2

    def block(k):
        first = (k % n) * share
        return array[first : first + share]

    own = [block(0), block(FAR), block(-FAR)]
    arrived = []
    for b in NEAR:
        parts = [block(b), block(b + FAR), block(b - FAR)]
        arrived.append(shift(jnp.concatenate(parts, axis=0).astype(BF16), Z, b))
    last = shift(block(half).astype(BF16), Z, half - FAR).astype(F32)
    sums = []
    for place in range(3):
        total = own[place]
        for piece in arrived:
            total = total + piece[place * share : (place + 1) * share].astype(F32)
        sums.append(total)
    up = shift((sums[1] + last).astype(BF16), Z, FAR)
    down = shift(sums[2].astype(BF16), Z, -FAR)
    return sums[0] + up.astype(F32) + down.astype(F32)


def gelu_tanh(values):
    return jax.nn.gelu(values, approximate=True)


def norm_back(upstream, unit_rows, inverse):
    unit_float = unit_rows.astype(F32)
    along = jnp.sum(unit_float * upstream, axis=-1, keepdims=True)
    return inverse * (upstream - unit_float * along)


def dot(a, b, dims):
    return lax.dot_general(a, b, (dims, ((), ())), preferred_element_type=F32)


def per_device(picture, caption, gain, entry, exit_matrix, mapping, scale, offset):
    rows = picture.shape[0]
    width = picture.shape[1]
    heads = lax.axis_size(MP)
    head_pos = lax.axis_index(MP)
    share = rows // heads
    cols = caption.shape[1]
    first_row = head_pos * share
    first_col = head_pos * cols
    text_part = dot(caption, mapping, ((1,), (0,))).astype(BF16)
    image_float = picture.astype(F32)
    mean_row = jnp.mean(image_float, axis=-1, keepdims=True)
    variance = jnp.mean((image_float - mean_row) ** 2, axis=-1, keepdims=True)
    inv_std = lax.rsqrt(variance + 1e-06)
    centred = (image_float - mean_row) * inv_std
    normed = (centred * gain).astype(BF16)
    preact = dot(normed, entry, ((1,), (0,)))
    hidden = gelu_tanh(preact).astype(BF16)
    partial_out = dot(hidden, exit_matrix, ((1,), (0,))).astype(BF16)
    own_rows = lax.dynamic_slice_in_dim(picture, first_row, share, 0).astype(F32)
    parts = [p.reshape(heads, share, width) for p in (text_part, partial_out)]
    sums = jnp.sum(swap(jnp.concatenate(parts, axis=1), MP).astype(F32), axis=0)
    text_out = sums[:share]
    inv_text = lax.rsqrt(jnp.sum(text_out * text_out, axis=-1, keepdims=True) + 1e-06)
    unit_text = (text_out * inv_text).astype(BF16)
    image_out = own_rows + sums[share:]
    inv_image = lax.rsqrt(jnp.sum(image_out * image_out, axis=-1, keepdims=True) + 1e-06)
    unit_image = (image_out * inv_image).astype(BF16)

    line = gathered_from_own(unit_text)
    texts = jnp.concatenate([line, exchange(line, "c", 1)], axis=0)
    images = spread(unit_image, XY)

    own_start = lax.axis_index(XY) * share
    text_ids = jnp.arange(texts.shape[0], dtype=jnp.int32)[:, None]
    image_ids = jnp.arange(images.shape[0], dtype=jnp.int32)[None, :] - own_start
    same = (text_ids == image_ids) & (text_ids < share)
    energies = scale * dot(texts, images, ((1,), (1,))) + offset
    polarity = jnp.where(same, 1.0, -1.0).astype(F32)
    weighted = (scale * -polarity * jax.nn.sigmoid(-polarity * energies)).astype(BF16)
    middle = weighted.shape[0] // 2
    text_sent = dot(weighted[middle:], images, ((1,), (0,))).astype(BF16)
    text_kept = dot(weighted[:middle], images, ((1,), (0,)))
    image_add = dot(weighted, texts, ((0,), (0,)))

    image_parts = swap(image_add.astype(BF16).reshape(-1, share, width), XY)
    image_dir = jnp.sum(image_parts.astype(F32), axis=0)
    grad_share = norm_back(image_dir, unit_image, inv_image).astype(BF16)
    grad_out_b = spread(grad_share, MP)

    swapped = exchange(text_sent, "c", 1)
    text_half = text_kept + swapped.astype(F32)
    text_dir = sum_over_line(text_half, share)
    grad_text_share = norm_back(text_dir, unit_text, inv_text).astype(BF16)

    grad_hidden = dot(grad_out_b, exit_matrix, ((1,), (1,)))
    _, pull_back = jax.vjp(gelu_tanh, preact)
    grad_pre = pull_back(grad_hidden)[0].astype(BF16)
    partial_normed = dot(grad_pre, entry, ((1,), (1,)))
    scaled_part = partial_normed * gain
    row_sums = jnp.stack(
        [jnp.sum(scaled_part, axis=-1), jnp.sum(scaled_part * centred, axis=-1)], axis=-1
    )
    sums_high = lax.reduce_precision(row_sums, 8, 7)
    sums_low = row_sums - sums_high
    sums_both = jnp.concatenate([sums_high, sums_low], axis=-1).astype(BF16)
    blocks = partial_normed.astype(BF16).reshape(rows, heads, cols).transpose(1, 0, 2)
    packed = jnp.concatenate(
        [blocks, jnp.broadcast_to(sums_both[None], (heads, *sums_both.shape))], axis=2
    )
    arrived = jnp.sum(swap(packed, MP).astype(F32), axis=0)
    means = (arrived[:, cols : cols + 2] + arrived[:, cols + 2 :]) / width
    gain_here = lax.dynamic_slice_in_dim(gain, first_col, cols, 0)
    feature = jnp.arange(width, dtype=jnp.int32)[:, None] - first_col
    chosen = (feature == jnp.arange(cols, dtype=jnp.int32)[None, :]).astype(BF16)
    picture_here = dot(picture, chosen, ((1,), (0,)))
    centred_here = (picture_here - mean_row) * inv_std
    grad_out_here = dot(grad_out_b, chosen, ((1,), (0,)))
    scaled = arrived[:, :cols] * gain_here
    grad_image = grad_out_here + inv_std * (
        scaled - means[:, :1] - centred_here * means[:, 1:]
    )
    grad_text = dot(spread(grad_text_share, MP), mapping, ((1,), (1,)))
    return (grad_image, grad_text)


def solution(mesh):
    split = Mesh(mesh.devices.reshape(4, 4, 2, 2, 4, 2), (*DP, *MP))
    in_specs = (
        P(DP, None),
        P(DP, MP),
        P(),
        P(None, MP),
        P(MP, None),
        P(MP, None),
        P(),
        P(),
    )
    out_specs = (P(DP, MP), P(DP, MP))
    return jax.shard_map(
        per_device, mesh=split, in_specs=in_specs, out_specs=out_specs, check_vma=False
    )
```

```python
import jax
import jax.numpy as jnp
from jax import lax
from jax.sharding import Mesh
from jax.sharding import PartitionSpec as P


DP = ("zh", "zl", "yl", "c")
MP = ("x", "yh")
Z = ("zh", "zl")
XY = ("yl", "x", "yh")
LINE = ("zh", "zl", "c")
NEAR = (1, 2)
FAR = (3, 6)
F32 = jnp.float32
BF16 = jnp.bfloat16


def swap(array, axes):
    return lax.all_to_all(array, axes, 0, 0, tiled=True)


def exchange(array, axes, k):
    n = lax.axis_size(axes)
    return lax.ppermute(array, axes, [(i, i ^ k) for i in range(n)])


def spread(array, axes):
    n = lax.axis_size(axes)
    copies = jnp.broadcast_to(array[None], (n, *array.shape))
    return swap(copies, axes).reshape(n * array.shape[0], *array.shape[1:])


def along(array, k):
    n = lax.axis_size(Z)
    moves = []
    for i in range(n):
        moves.append((2 * i, 2 * ((i - k) % n)))
        moves.append((2 * i + 1, 2 * ((i + k) % n) + 1))
    return lax.ppermute(array, LINE, moves)


def gathered_line(array):
    share = array.shape[0]
    pair = jnp.concatenate([array, exchange(array, "c", 1)], axis=0)
    far = [along(pair, -k) for k in FAR]
    near = jnp.concatenate([pair, *far], axis=0)
    cut = near.shape[0] - share
    last = [along(near, -NEAR[0]), along(near[:cut], -NEAR[1])]
    mine = jnp.concatenate([near, *last], axis=0)
    other = exchange(mine[2 * share :], "c", 1)
    return jnp.concatenate([mine, other], axis=0)


def summed_line(kept, swapped, share):
    pair = 2 * share
    rest = kept[pair:] + swapped.astype(F32)
    cut = 5 * pair
    one = along(rest[2 * pair : cut].astype(BF16), NEAR[0]).astype(F32)
    two = along(rest[cut:].astype(BF16), NEAR[1]).astype(F32)
    here = kept[:pair] + one[:pair] + two[:pair]
    third = rest[:pair] + one[pair : 2 * pair] + two[pair : 2 * pair]
    sixth = rest[pair : 2 * pair] + one[2 * pair :]
    sixth = jnp.concatenate([sixth[:share] + two[2 * pair :], sixth[share:]], axis=0)
    three = along(third.astype(BF16), FAR[0])
    six = along(sixth.astype(BF16), FAR[1])
    total = here + three.astype(F32) + six.astype(F32)
    partner = exchange(total[share:].astype(BF16), "c", 1)
    return total[:share] + partner.astype(F32)


def gelu_tanh(values):
    return jax.nn.gelu(values, approximate=True)


def norm_back(upstream, unit_rows, inverse):
    unit_float = unit_rows.astype(F32)
    along = jnp.sum(unit_float * upstream, axis=-1, keepdims=True)
    return inverse * (upstream - unit_float * along)


def dot(a, b, dims):
    return lax.dot_general(a, b, (dims, ((), ())), preferred_element_type=F32)


def per_device(picture, caption, gain, entry, exit_matrix, mapping, scale, offset):
    rows = picture.shape[0]
    width = picture.shape[1]
    heads = lax.axis_size(MP)
    head_pos = lax.axis_index(MP)
    share = rows // heads
    cols = caption.shape[1]
    first_row = head_pos * share
    first_col = head_pos * cols
    text_part = dot(caption, mapping, ((1,), (0,))).astype(BF16)
    image_float = picture.astype(F32)
    mean_row = jnp.mean(image_float, axis=-1, keepdims=True)
    variance = jnp.mean((image_float - mean_row) ** 2, axis=-1, keepdims=True)
    inv_std = lax.rsqrt(variance + 1e-06)
    centred = (image_float - mean_row) * inv_std
    normed = (centred * gain).astype(BF16)
    preact = dot(normed, entry, ((1,), (0,)))
    hidden = gelu_tanh(preact).astype(BF16)
    partial_out = dot(hidden, exit_matrix, ((1,), (0,))).astype(BF16)
    own_rows = lax.dynamic_slice_in_dim(picture, first_row, share, 0).astype(F32)
    parts = [p.reshape(heads, share, width) for p in (text_part, partial_out)]
    sums = jnp.sum(swap(jnp.concatenate(parts, axis=1), MP).astype(F32), axis=0)
    text_out = sums[:share]
    inv_text = lax.rsqrt(jnp.sum(text_out * text_out, axis=-1, keepdims=True) + 1e-06)
    unit_text = (text_out * inv_text).astype(BF16)
    image_out = own_rows + sums[share:]
    inv_image = lax.rsqrt(jnp.sum(image_out * image_out, axis=-1, keepdims=True) + 1e-06)
    unit_image = (image_out * inv_image).astype(BF16)

    texts = gathered_line(unit_text)
    images = spread(unit_image, XY)

    own_start = lax.axis_index(XY) * share
    text_ids = jnp.arange(texts.shape[0], dtype=jnp.int32)[:, None]
    image_ids = jnp.arange(images.shape[0], dtype=jnp.int32)[None, :] - own_start
    same = (text_ids == image_ids) & (text_ids < share)
    energies = scale * dot(texts, images, ((1,), (1,))) + offset
    polarity = jnp.where(same, 1.0, -1.0).astype(F32)
    weighted = (scale * -polarity * jax.nn.sigmoid(-polarity * energies)).astype(BF16)
    middle = weighted.shape[0] // 2 + share
    text_sent = dot(weighted[middle:], images, ((1,), (0,))).astype(BF16)
    text_kept = dot(weighted[:middle], images, ((1,), (0,)))
    image_add = dot(weighted, texts, ((0,), (0,)))

    image_parts = swap(image_add.astype(BF16).reshape(-1, share, width), XY)
    image_dir = jnp.sum(image_parts.astype(F32), axis=0)
    grad_share = norm_back(image_dir, unit_image, inv_image).astype(BF16)
    grad_out_b = spread(grad_share, MP)

    swapped = exchange(text_sent, "c", 1)
    text_dir = summed_line(text_kept, swapped, share)
    grad_text_share = norm_back(text_dir, unit_text, inv_text).astype(BF16)

    grad_hidden = dot(grad_out_b, exit_matrix, ((1,), (1,)))
    _, pull_back = jax.vjp(gelu_tanh, preact)
    grad_pre = pull_back(grad_hidden)[0].astype(BF16)
    partial_normed = dot(grad_pre, entry, ((1,), (1,)))
    scaled_part = partial_normed * gain
    row_sums = jnp.stack(
        [jnp.sum(scaled_part, axis=-1), jnp.sum(scaled_part * centred, axis=-1)], axis=-1
    )
    sums_high = lax.reduce_precision(row_sums, 8, 7)
    sums_low = row_sums - sums_high
    sums_both = jnp.concatenate([sums_high, sums_low], axis=-1).astype(BF16)
    blocks = partial_normed.astype(BF16).reshape(rows, heads, cols).transpose(1, 0, 2)
    packed = jnp.concatenate(
        [blocks, jnp.broadcast_to(sums_both[None], (heads, *sums_both.shape))], axis=2
    )
    arrived = jnp.sum(swap(packed, MP).astype(F32), axis=0)
    means = (arrived[:, cols : cols + 2] + arrived[:, cols + 2 :]) / width
    gain_here = lax.dynamic_slice_in_dim(gain, first_col, cols, 0)
    feature = jnp.arange(width, dtype=jnp.int32)[:, None] - first_col
    chosen = (feature == jnp.arange(cols, dtype=jnp.int32)[None, :]).astype(BF16)
    picture_here = dot(picture, chosen, ((1,), (0,)))
    centred_here = (picture_here - mean_row) * inv_std
    grad_out_here = dot(grad_out_b, chosen, ((1,), (0,)))
    scaled = arrived[:, :cols] * gain_here
    grad_image = grad_out_here + inv_std * (
        scaled - means[:, :1] - centred_here * means[:, 1:]
    )
    grad_text = dot(spread(grad_text_share, MP), mapping, ((1,), (1,)))
    return (grad_image, grad_text)


def solution(mesh):
    split = Mesh(mesh.devices.reshape(4, 4, 2, 2, 4, 2), (*DP, *MP))
    in_specs = (
        P(DP, None),
        P(DP, MP),
        P(),
        P(None, MP),
        P(MP, None),
        P(MP, None),
        P(),
        P(),
    )
    out_specs = (P(DP, MP), P(DP, MP))
    return jax.shard_map(
        per_device, mesh=split, in_specs=in_specs, out_specs=out_specs, check_vma=False
    )
```

```python
import jax
import jax.numpy as jnp
from jax import lax
from jax.experimental import pallas as pl
from jax.sharding import Mesh
from jax.sharding import PartitionSpec as P


DP = ("zh", "zl", "yl", "c")
MP = ("x", "yh")
Z = ("zh", "zl")
XY = ("yl", "x", "yh")
LINE = ("zh", "zl", "c")
NEAR = (1, 2)
FAR = (3, 6)
F32 = jnp.float32
BF16 = jnp.bfloat16


def swap(array, axes):
    return lax.all_to_all(array, axes, 0, 0, tiled=True)


def exchange(array, axes, k):
    n = lax.axis_size(axes)
    return lax.ppermute(array, axes, [(i, i ^ k) for i in range(n)])


def spread(array, axes):
    n = lax.axis_size(axes)
    copies = jnp.broadcast_to(array[None], (n, *array.shape))
    return swap(copies, axes).reshape(n * array.shape[0], *array.shape[1:])


def along(array, k):
    n = lax.axis_size(Z)
    moves = []
    for i in range(n):
        moves.append((2 * i, 2 * ((i - k) % n)))
        moves.append((2 * i + 1, 2 * ((i + k) % n) + 1))
    return lax.ppermute(array, LINE, moves)


def gathered_line(array):
    share = array.shape[0]
    pair = jnp.concatenate([array, exchange(array, "c", 1)], axis=0)
    far = [along(pair, -k) for k in FAR]
    near = jnp.concatenate([pair, *far], axis=0)
    cut = near.shape[0] - share
    last = [along(near, -NEAR[0]), along(near[:cut], -NEAR[1])]
    mine = jnp.concatenate([near, *last], axis=0)
    other = exchange(mine[2 * share :], "c", 1)
    return jnp.concatenate([mine, other], axis=0)


def summed_line(kept, swapped, share):
    pair = 2 * share
    rest = kept[pair:] + swapped.astype(F32)
    cut = 5 * pair
    one = along(rest[2 * pair : cut].astype(BF16), NEAR[0]).astype(F32)
    two = along(rest[cut:].astype(BF16), NEAR[1]).astype(F32)
    here = kept[:pair] + one[:pair] + two[:pair]
    third = rest[:pair] + one[pair : 2 * pair] + two[pair : 2 * pair]
    sixth = rest[pair : 2 * pair] + one[2 * pair :]
    sixth = jnp.concatenate([sixth[:share] + two[2 * pair :], sixth[share:]], axis=0)
    three = along(third.astype(BF16), FAR[0])
    six = along(sixth.astype(BF16), FAR[1])
    total = here + three.astype(F32) + six.astype(F32)
    partner = exchange(total[share:].astype(BF16), "c", 1)
    return total[:share] + partner.astype(F32)


LANES = 128
SUM_ROWS = 16


def pack_kernel(back_ref, sums_ref, text_ref, out_ref):
    heads = out_ref.shape[0]
    cols = back_ref.shape[0] // heads
    rows = back_ref.shape[1]
    share, width = text_ref.shape
    for h in range(heads):
        block = back_ref[h * cols : (h + 1) * cols, :]
        out_ref[h, :cols, :] = block[:, :LANES]
        out_ref[h, cols : 2 * cols, : rows - LANES] = block[:, LANES:]
        out_ref[h, cols : 2 * cols, rows - LANES :] = jnp.zeros((cols, 2 * LANES - rows), BF16)
        out_ref[h, 2 * cols : 2 * cols + SUM_ROWS, :] = sums_ref[...]
        for k in range(width // LANES):
            first = 2 * cols + SUM_ROWS + k * share
            out_ref[h, first : first + share, :] = text_ref[:, k * LANES : (k + 1) * LANES]


def finish_kernel(
    packed_ref, direct_ref, centred_ref, inv_ref, gain_ref, mapping_ref, image_ref, text_ref, rows_ref
):
    heads = packed_ref.shape[0]
    cols, rows = direct_ref.shape
    width = mapping_ref.shape[1]
    share = rows // heads
    sums = packed_ref[0, 2 * cols : 2 * cols + SUM_ROWS, :].astype(F32)
    for h in range(1, heads):
        sums = sums + packed_ref[h, 2 * cols : 2 * cols + SUM_ROWS, :].astype(F32)
    for half, span in enumerate((LANES, rows - LANES)):
        here = slice(half * LANES, half * LANES + span)
        total = packed_ref[0, half * cols : (half + 1) * cols, :span].astype(F32)
        for h in range(1, heads):
            total = total + packed_ref[h, half * cols : (half + 1) * cols, :span].astype(F32)
        one = (sums[half : half + 1, :span] + sums[half + 4 : half + 5, :span]) / width
        two = (sums[half + 2 : half + 3, :span] + sums[half + 6 : half + 7, :span]) / width
        image_ref[:, here] = direct_ref[:, here] + inv_ref[:, here] * (
            total * gain_ref[...] - one - centred_ref[:, here] * two
        )
    for h in range(heads):
        for k in range(width // LANES):
            first = 2 * cols + SUM_ROWS + k * share
            rows_ref[h * share : (h + 1) * share, k * LANES : (k + 1) * LANES] = packed_ref[
                h, first : first + share, :
            ]
    text_ref[...] = lax.dot_general(
        mapping_ref[...],
        rows_ref[...],
        (((1,), (1,)), ((), ())),
        preferred_element_type=F32,
    )


def gelu_tanh(values):
    return jax.nn.gelu(values, approximate=True)


def norm_back(upstream, unit_rows, inverse):
    unit_float = unit_rows.astype(F32)
    along = jnp.sum(unit_float * upstream, axis=-1, keepdims=True)
    return inverse * (upstream - unit_float * along)


def dot(a, b, dims):
    return lax.dot_general(a, b, (dims, ((), ())), preferred_element_type=F32)


def per_device(picture, caption, gain, entry, exit_matrix, mapping, scale, offset):
    rows = picture.shape[0]
    width = picture.shape[1]
    heads = lax.axis_size(MP)
    head_pos = lax.axis_index(MP)
    share = rows // heads
    cols = caption.shape[1]
    first_row = head_pos * share
    first_col = head_pos * cols
    text_part = dot(caption, mapping, ((1,), (0,))).astype(BF16)
    image_float = picture.astype(F32)
    mean_row = jnp.mean(image_float, axis=-1, keepdims=True)
    variance = jnp.mean((image_float - mean_row) ** 2, axis=-1, keepdims=True)
    inv_std = lax.rsqrt(variance + 1e-06)
    centred = (image_float - mean_row) * inv_std
    normed = (centred * gain).astype(BF16)
    preact = dot(normed, entry, ((1,), (0,)))
    entry_gain = jnp.sum(entry.astype(F32) * gain[:, None], axis=0)
    hidden = gelu_tanh(preact).astype(BF16)
    partial_out = dot(hidden, exit_matrix, ((1,), (0,))).astype(BF16)
    own_rows = lax.dynamic_slice_in_dim(picture, first_row, share, 0).astype(F32)
    parts = [p.reshape(heads, share, width) for p in (text_part, partial_out)]
    sums = jnp.sum(swap(jnp.concatenate(parts, axis=1), MP).astype(F32), axis=0)
    text_out = sums[:share]
    inv_text = lax.rsqrt(jnp.sum(text_out * text_out, axis=-1, keepdims=True) + 1e-06)
    unit_text = (text_out * inv_text).astype(BF16)
    image_out = own_rows + sums[share:]
    inv_image = lax.rsqrt(jnp.sum(image_out * image_out, axis=-1, keepdims=True) + 1e-06)
    unit_image = (image_out * inv_image).astype(BF16)

    texts = gathered_line(unit_text)
    images = spread(unit_image, XY)

    own_start = lax.axis_index(XY) * share
    text_ids = jnp.arange(texts.shape[0], dtype=jnp.int32)[:, None]
    image_ids = jnp.arange(images.shape[0], dtype=jnp.int32)[None, :] - own_start
    same = (text_ids == image_ids) & (text_ids < share)
    energies = scale * dot(texts, images, ((1,), (1,))) + offset
    polarity = jnp.where(same, 1.0, -1.0).astype(F32)
    weighted = (scale * -polarity * jax.nn.sigmoid(-polarity * energies)).astype(BF16)
    middle = weighted.shape[0] // 2 + share
    text_sent = dot(weighted[middle:], images, ((1,), (0,))).astype(BF16)
    text_kept = dot(weighted[:middle], images, ((1,), (0,)))
    image_add = dot(weighted, texts, ((0,), (0,)))

    image_parts = swap(image_add.astype(BF16).reshape(-1, share, width), XY)
    image_dir = jnp.sum(image_parts.astype(F32), axis=0)
    grad_share = norm_back(image_dir, unit_image, inv_image).astype(BF16)
    grad_out_b = spread(grad_share, MP)

    swapped = exchange(text_sent, "c", 1)
    text_dir = summed_line(text_kept, swapped, share)
    grad_text_share = norm_back(text_dir, unit_text, inv_text).astype(BF16)

    grad_hidden = dot(grad_out_b, exit_matrix, ((1,), (1,)))
    unused, pull_back = jax.vjp(gelu_tanh, preact)
    grad_pre = pull_back(grad_hidden)[0].astype(BF16)
    back = dot(entry, grad_pre, ((1,), (1,))).astype(BF16)
    pre_float = grad_pre.astype(F32)
    row_sums = jnp.stack(
        [jnp.sum(pre_float * entry_gain, axis=-1), jnp.sum(pre_float * preact, axis=-1)]
    )
    sums_high = lax.reduce_precision(row_sums, 8, 7)
    sums_low = row_sums - sums_high
    sums_both = jnp.concatenate([sums_high, sums_low], axis=0).astype(BF16)
    sums_both = jnp.pad(sums_both, ((0, 0), (0, 2 * LANES - rows))).reshape(-1, LANES)
    sums_both = jnp.pad(sums_both, ((0, SUM_ROWS - sums_both.shape[0]), (0, 0)))
    length = 2 * cols + SUM_ROWS + share * width // LANES
    packed = pl.pallas_call(
        pack_kernel, out_shape=jax.ShapeDtypeStruct((heads, length, LANES), BF16)
    )(back, sums_both, grad_text_share)
    arrived = swap(packed, MP)
    gain_here = lax.dynamic_slice_in_dim(gain, first_col, cols, 0)
    feature = jnp.arange(width, dtype=jnp.int32)[None, :] - first_col
    chosen = (feature == jnp.arange(cols, dtype=jnp.int32)[:, None]).astype(BF16)
    picture_here = dot(chosen, picture, ((1,), (1,)))
    centred_here = (picture_here - mean_row.T) * inv_std.T
    direct = dot(chosen, grad_out_b, ((1,), (1,)))
    outs = jax.ShapeDtypeStruct((cols, rows), F32)
    grad_image, grad_text, unused = pl.pallas_call(
        finish_kernel, out_shape=(outs, outs, jax.ShapeDtypeStruct((rows, width), BF16))
    )(arrived, direct, centred_here, inv_std.T, gain_here[:, None], mapping)
    return (grad_image.T, grad_text.T)


def solution(mesh):
    split = Mesh(mesh.devices.reshape(4, 4, 2, 2, 4, 2), (*DP, *MP))
    in_specs = (
        P(DP, None),
        P(DP, MP),
        P(),
        P(None, MP),
        P(MP, None),
        P(MP, None),
        P(),
        P(),
    )
    out_specs = (P(DP, MP), P(DP, MP))
    return jax.shard_map(
        per_device, mesh=split, in_specs=in_specs, out_specs=out_specs, check_vma=False
    )
```

```python
import functools

import jax
import jax.numpy as jnp
from jax import lax
from jax.experimental import pallas as pl
from jax.experimental.pallas import tpu as pltpu
from jax.sharding import Mesh
from jax.sharding import PartitionSpec as P


DP = ("zh", "zl", "yl", "c")
MP = ("x", "yh")
Z = ("zh", "zl")
XY = ("yl", "x", "yh")
LINE = ("zh", "zl", "c")
NEAR = (1, 2)
FAR = (3, 6)
F32 = jnp.float32
BF16 = jnp.bfloat16


def swap(array, axes):
    return lax.all_to_all(array, axes, 0, 0, tiled=True)


def exchange(array, axes, k):
    n = lax.axis_size(axes)
    return lax.ppermute(array, axes, [(i, i ^ k) for i in range(n)])


def spread(array, axes):
    n = lax.axis_size(axes)
    copies = jnp.broadcast_to(array[None], (n, *array.shape))
    return swap(copies, axes).reshape(n * array.shape[0], *array.shape[1:])


def along(array, k):
    n = lax.axis_size(Z)
    moves = []
    for i in range(n):
        moves.append((2 * i, 2 * ((i - k) % n)))
        moves.append((2 * i + 1, 2 * ((i + k) % n) + 1))
    return lax.ppermute(array, LINE, moves)


def gathered_line(array):
    share = array.shape[0]
    pair = jnp.concatenate([array, exchange(array, "c", 1)], axis=0)
    far = [along(pair, -k) for k in FAR]
    near = jnp.concatenate([pair, *far], axis=0)
    cut = near.shape[0] - share
    last = [along(near, -NEAR[0]), along(near[:cut], -NEAR[1])]
    other = exchange(jnp.concatenate([*far, *last], axis=0), "c", 1)
    return [pair, *far, *last, other]


def shape(rows, width, dtype):
    return jax.ShapeDtypeStruct((rows, width), dtype)


def pairs_kernel(share, consts_ref, start_ref, *refs):
    pieces, images_ref = refs[:6], refs[6]
    sent_ref, kept_ref, image_ref, texts_ref, weights_ref = refs[7:]
    at = 0
    for piece in pieces:
        texts_ref[at : at + piece.shape[0], :] = piece[...]
        at += piece.shape[0]
    scale = consts_ref[0]
    step = at // 6
    columns = images_ref.shape[0]
    for first in range(0, at, step):
        energies = scale * dot(
            texts_ref[first : first + step, :], images_ref[...], ((1,), (1,))
        ) + consts_ref[1]
        if first:
            weights = scale * jax.nn.sigmoid(energies)
        else:
            text_ids = lax.broadcasted_iota(jnp.int32, (step, columns), 0)
            image_ids = lax.broadcasted_iota(jnp.int32, (step, columns), 1) - start_ref[0]
            same = (text_ids == image_ids) & (text_ids < share)
            polarity = jnp.where(same, 1.0, -1.0).astype(F32)
            weights = scale * -polarity * jax.nn.sigmoid(-polarity * energies)
        weights_ref[first : first + step, :] = weights.astype(BF16)
    middle = kept_ref.shape[0]
    sent_ref[...] = dot(weights_ref[middle:, :], images_ref[...], ((1,), (0,))).astype(BF16)
    kept_ref[...] = dot(weights_ref[:middle, :], images_ref[...], ((1,), (0,)))
    image_ref[...] = dot(weights_ref[...], texts_ref[...], ((0,), (0,))).astype(BF16)


def near_kernel(kept_ref, swapped_ref, one_ref, two_ref):
    long = one_ref.shape[0]
    pair = long // 3
    one_ref[...] = (
        kept_ref[3 * pair : 6 * pair, :] + swapped_ref[2 * pair : 5 * pair, :].astype(F32)
    ).astype(BF16)
    two_ref[...] = (
        kept_ref[6 * pair :, :] + swapped_ref[5 * pair :, :].astype(F32)
    ).astype(BF16)


def far_kernel(kept_ref, swapped_ref, one_ref, two_ref, here_ref, three_ref, six_ref):
    pair = here_ref.shape[0]
    share = pair // 2
    here_ref[...] = (
        kept_ref[:pair, :] + one_ref[:pair, :].astype(F32) + two_ref[:pair, :].astype(F32)
    )
    three_ref[...] = (
        kept_ref[pair : 2 * pair, :]
        + swapped_ref[:pair, :].astype(F32)
        + one_ref[pair : 2 * pair, :].astype(F32)
        + two_ref[pair : 2 * pair, :].astype(F32)
    ).astype(BF16)
    sixth = (
        kept_ref[2 * pair : 3 * pair, :]
        + swapped_ref[pair : 2 * pair, :].astype(F32)
        + one_ref[2 * pair :, :].astype(F32)
    )
    own = sixth[:share, :] + two_ref[2 * pair :, :].astype(F32)
    six_ref[:share, :] = own.astype(BF16)
    six_ref[share:, :] = sixth[share:, :].astype(BF16)


def last_kernel(here_ref, three_ref, six_ref, own_ref, partner_ref):
    share = own_ref.shape[0]
    total = here_ref[...] + three_ref[...].astype(F32) + six_ref[...].astype(F32)
    own_ref[...] = total[:share, :]
    partner_ref[...] = total[share:, :].astype(BF16)


def summed_line(kept, swapped, share):
    width = kept.shape[1]
    pair = 2 * share
    one, two = pl.pallas_call(
        near_kernel,
        out_shape=(shape(3 * pair, width, BF16), shape(2 * pair + share, width, BF16)),
    )(kept, swapped)
    one = along(one, NEAR[0])
    two = along(two, NEAR[1])
    here, three, six = pl.pallas_call(
        far_kernel,
        out_shape=(shape(pair, width, F32), shape(pair, width, BF16), shape(pair, width, BF16)),
    )(kept, swapped, one, two)
    three = along(three, FAR[0])
    six = along(six, FAR[1])
    own, partner = pl.pallas_call(
        last_kernel, out_shape=(shape(share, width, F32), shape(share, width, BF16))
    )(here, three, six)
    partner = exchange(partner, "c", 1)
    return own + partner.astype(F32)


LANES = 128
SUM_ROWS = 16


def pack_kernel(back_ref, sums_ref, text_ref, out_ref):
    heads = out_ref.shape[0]
    cols = back_ref.shape[0] // heads
    rows = back_ref.shape[1]
    share, width = text_ref.shape
    for h in range(heads):
        block = back_ref[h * cols : (h + 1) * cols, :]
        out_ref[h, :cols, :] = block[:, :LANES]
        out_ref[h, cols : 2 * cols, : rows - LANES] = block[:, LANES:]
        out_ref[h, cols : 2 * cols, rows - LANES :] = jnp.zeros((cols, 2 * LANES - rows), BF16)
        out_ref[h, 2 * cols : 2 * cols + SUM_ROWS, :] = sums_ref[...]
        for k in range(width // LANES):
            first = 2 * cols + SUM_ROWS + k * share
            out_ref[h, first : first + share, :] = text_ref[:, k * LANES : (k + 1) * LANES]


def finish_kernel(
    packed_ref, direct_ref, centred_ref, inv_ref, gain_ref, mapping_ref, image_ref, text_ref, rows_ref
):
    heads = packed_ref.shape[0]
    cols, rows = direct_ref.shape
    width = mapping_ref.shape[1]
    share = rows // heads
    sums = packed_ref[0, 2 * cols : 2 * cols + SUM_ROWS, :].astype(F32)
    for h in range(1, heads):
        sums = sums + packed_ref[h, 2 * cols : 2 * cols + SUM_ROWS, :].astype(F32)
    for half, span in enumerate((LANES, rows - LANES)):
        here = slice(half * LANES, half * LANES + span)
        total = packed_ref[0, half * cols : (half + 1) * cols, :span].astype(F32)
        for h in range(1, heads):
            total = total + packed_ref[h, half * cols : (half + 1) * cols, :span].astype(F32)
        one = (sums[half : half + 1, :span] + sums[half + 4 : half + 5, :span]) / width
        two = (sums[half + 2 : half + 3, :span] + sums[half + 6 : half + 7, :span]) / width
        image_ref[:, here] = direct_ref[:, here] + inv_ref[:, here] * (
            total * gain_ref[...] - one - centred_ref[:, here] * two
        )
    for h in range(heads):
        for k in range(width // LANES):
            first = 2 * cols + SUM_ROWS + k * share
            rows_ref[h * share : (h + 1) * share, k * LANES : (k + 1) * LANES] = packed_ref[
                h, first : first + share, :
            ]
    text_ref[...] = lax.dot_general(
        mapping_ref[...],
        rows_ref[...],
        (((1,), (1,)), ((), ())),
        preferred_element_type=F32,
    )


def gelu_tanh(values):
    return jax.nn.gelu(values, approximate=True)


def norm_back(upstream, unit_rows, inverse):
    unit_float = unit_rows.astype(F32)
    along = jnp.sum(unit_float * upstream, axis=-1, keepdims=True)
    return inverse * (upstream - unit_float * along)


def dot(a, b, dims):
    return lax.dot_general(a, b, (dims, ((), ())), preferred_element_type=F32)


def per_device(picture, caption, gain, entry, exit_matrix, mapping, scale, offset):
    rows = picture.shape[0]
    width = picture.shape[1]
    heads = lax.axis_size(MP)
    head_pos = lax.axis_index(MP)
    share = rows // heads
    cols = caption.shape[1]
    first_row = head_pos * share
    first_col = head_pos * cols
    text_part = dot(caption, mapping, ((1,), (0,))).astype(BF16)
    image_float = picture.astype(F32)
    mean_row = jnp.mean(image_float, axis=-1, keepdims=True)
    variance = jnp.mean((image_float - mean_row) ** 2, axis=-1, keepdims=True)
    inv_std = lax.rsqrt(variance + 1e-06)
    centred = (image_float - mean_row) * inv_std
    normed = (centred * gain).astype(BF16)
    preact = dot(normed, entry, ((1,), (0,)))
    entry_gain = jnp.sum(entry.astype(F32) * gain[:, None], axis=0)
    hidden = gelu_tanh(preact).astype(BF16)
    partial_out = dot(hidden, exit_matrix, ((1,), (0,))).astype(BF16)
    own_rows = lax.dynamic_slice_in_dim(picture, first_row, share, 0).astype(F32)
    parts = [p.reshape(heads, share, width) for p in (text_part, partial_out)]
    sums = jnp.sum(swap(jnp.concatenate(parts, axis=1), MP).astype(F32), axis=0)
    text_out = sums[:share]
    inv_text = lax.rsqrt(jnp.sum(text_out * text_out, axis=-1, keepdims=True) + 1e-06)
    unit_text = (text_out * inv_text).astype(BF16)
    image_out = own_rows + sums[share:]
    inv_image = lax.rsqrt(jnp.sum(image_out * image_out, axis=-1, keepdims=True) + 1e-06)
    unit_image = (image_out * inv_image).astype(BF16)

    pieces = gathered_line(unit_text)
    images = spread(unit_image, XY)

    own_start = (lax.axis_index(XY) * share).reshape(1)
    consts = jnp.stack([scale, offset])
    sent_rows = pieces[-1].shape[0]
    kept_rows = sum(p.shape[0] for p in pieces) - sent_rows
    scalars = pl.BlockSpec(memory_space=pltpu.SMEM)
    whole = pl.BlockSpec(memory_space=pltpu.VMEM)
    text_sent, text_kept, image_add = pl.pallas_call(
        functools.partial(pairs_kernel, share),
        in_specs=[scalars, scalars] + [whole] * 7,
        out_shape=(
            shape(sent_rows, width, BF16),
            shape(kept_rows, width, F32),
            shape(images.shape[0], width, BF16),
        ),
        scratch_shapes=[
            pltpu.VMEM((sent_rows + kept_rows, width), BF16),
            pltpu.VMEM((sent_rows + kept_rows, images.shape[0]), BF16),
        ],
    )(consts, own_start, *pieces, images)

    image_parts = swap(image_add.reshape(-1, share, width), XY)
    image_dir = jnp.sum(image_parts.astype(F32), axis=0)
    grad_share = norm_back(image_dir, unit_image, inv_image).astype(BF16)
    grad_out_b = spread(grad_share, MP)

    swapped = exchange(text_sent, "c", 1)
    text_dir = summed_line(text_kept, swapped, share)
    grad_text_share = norm_back(text_dir, unit_text, inv_text).astype(BF16)

    grad_hidden = dot(grad_out_b, exit_matrix, ((1,), (1,)))
    unused, pull_back = jax.vjp(gelu_tanh, preact)
    grad_pre = pull_back(grad_hidden)[0].astype(BF16)
    back = dot(entry, grad_pre, ((1,), (1,))).astype(BF16)
    pre_float = grad_pre.astype(F32)
    row_sums = jnp.stack(
        [jnp.sum(pre_float * entry_gain, axis=-1), jnp.sum(pre_float * preact, axis=-1)]
    )
    sums_high = lax.reduce_precision(row_sums, 8, 7)
    sums_low = row_sums - sums_high
    sums_both = jnp.concatenate([sums_high, sums_low], axis=0).astype(BF16)
    sums_both = jnp.pad(sums_both, ((0, 0), (0, 2 * LANES - rows))).reshape(-1, LANES)
    sums_both = jnp.pad(sums_both, ((0, SUM_ROWS - sums_both.shape[0]), (0, 0)))
    length = 2 * cols + SUM_ROWS + share * width // LANES
    packed = pl.pallas_call(
        pack_kernel, out_shape=jax.ShapeDtypeStruct((heads, length, LANES), BF16)
    )(back, sums_both, grad_text_share)
    arrived = swap(packed, MP)
    gain_here = lax.dynamic_slice_in_dim(gain, first_col, cols, 0)
    feature = jnp.arange(width, dtype=jnp.int32)[None, :] - first_col
    chosen = (feature == jnp.arange(cols, dtype=jnp.int32)[:, None]).astype(BF16)
    picture_here = dot(chosen, picture, ((1,), (1,)))
    centred_here = (picture_here - mean_row.T) * inv_std.T
    direct = dot(chosen, grad_out_b, ((1,), (1,)))
    outs = jax.ShapeDtypeStruct((cols, rows), F32)
    grad_image, grad_text, unused = pl.pallas_call(
        finish_kernel, out_shape=(outs, outs, jax.ShapeDtypeStruct((rows, width), BF16))
    )(arrived, direct, centred_here, inv_std.T, gain_here[:, None], mapping)
    return (grad_image.T, grad_text.T)


def solution(mesh):
    split = Mesh(mesh.devices.reshape(4, 4, 2, 2, 4, 2), (*DP, *MP))
    in_specs = (
        P(DP, None),
        P(DP, MP),
        P(),
        P(None, MP),
        P(MP, None),
        P(MP, None),
        P(),
        P(),
    )
    out_specs = (P(DP, MP), P(DP, MP))
    return jax.shard_map(
        per_device, mesh=split, in_specs=in_specs, out_specs=out_specs, check_vma=False
    )
```

```python
import functools

import jax
import jax.numpy as jnp
from jax import lax
from jax.experimental import pallas as pl
from jax.experimental.pallas import tpu as pltpu
from jax.sharding import Mesh
from jax.sharding import PartitionSpec as P


DP = ("zh", "zl", "yl", "c")
MP = ("x", "yh")
Z = ("zh", "zl")
XY = ("yl", "x", "yh")
LINE = ("zh", "zl", "c")
NEAR = (1, 2)
FAR = (3, 6)
F32 = jnp.float32
BF16 = jnp.bfloat16


def swap(array, axes):
    return lax.all_to_all(array, axes, 0, 0, tiled=True)


def exchange(array, axes, k):
    n = lax.axis_size(axes)
    return lax.ppermute(array, axes, [(i, i ^ k) for i in range(n)])


def spread(array, axes):
    n = lax.axis_size(axes)
    copies = jnp.broadcast_to(array[None], (n, *array.shape))
    return swap(copies, axes).reshape(n * array.shape[0], *array.shape[1:])


def along(array, k):
    n = lax.axis_size(Z)
    moves = []
    for i in range(n):
        moves.append((2 * i, 2 * ((i - k) % n)))
        moves.append((2 * i + 1, 2 * ((i + k) % n) + 1))
    return lax.ppermute(array, LINE, moves)


def gathered_line(array):
    share = array.shape[0]
    pair = jnp.concatenate([array, exchange(array, "c", 1)], axis=0)
    third = along(pair, -FAR[0])
    far = [third, along(third, FAR[0] - FAR[1])]
    near = jnp.concatenate([pair, *far], axis=0)
    cut = near.shape[0] - share
    last = [along(near, -NEAR[0]), along(near[:cut], -NEAR[1])]
    other = exchange(jnp.concatenate([*far, *last], axis=0), "c", 1)
    return [pair, *far, *last, other]


def shape(rows, width, dtype):
    return jax.ShapeDtypeStruct((rows, width), dtype)


def pairs_kernel(share, consts_ref, start_ref, *refs):
    pieces, images_ref = refs[:6], refs[6]
    sent_ref, kept_ref, image_ref, texts_ref, weights_ref = refs[7:]
    at = 0
    for piece in pieces:
        texts_ref[at : at + piece.shape[0], :] = piece[...]
        at += piece.shape[0]
    scale = consts_ref[0]
    step = at // 6
    columns = images_ref.shape[0]
    for first in range(0, at, step):
        energies = scale * dot(
            texts_ref[first : first + step, :], images_ref[...], ((1,), (1,))
        ) + consts_ref[1]
        if first:
            weights = scale * jax.nn.sigmoid(energies)
        else:
            text_ids = lax.broadcasted_iota(jnp.int32, (step, columns), 0)
            image_ids = lax.broadcasted_iota(jnp.int32, (step, columns), 1) - start_ref[0]
            same = (text_ids == image_ids) & (text_ids < share)
            polarity = jnp.where(same, 1.0, -1.0).astype(F32)
            weights = scale * -polarity * jax.nn.sigmoid(-polarity * energies)
        weights_ref[first : first + step, :] = weights.astype(BF16)
    middle = kept_ref.shape[0]
    sent_ref[...] = dot(weights_ref[middle:, :], images_ref[...], ((1,), (0,))).astype(BF16)
    kept_ref[...] = dot(weights_ref[:middle, :], images_ref[...], ((1,), (0,)))
    image_ref[...] = dot(weights_ref[...], texts_ref[...], ((0,), (0,))).astype(BF16)


def near_kernel(kept_ref, swapped_ref, one_ref, two_ref):
    long = one_ref.shape[0]
    pair = long // 3
    one_ref[...] = (
        kept_ref[3 * pair : 6 * pair, :] + swapped_ref[2 * pair : 5 * pair, :].astype(F32)
    ).astype(BF16)
    two_ref[...] = (
        kept_ref[6 * pair :, :] + swapped_ref[5 * pair :, :].astype(F32)
    ).astype(BF16)


def far_kernel(kept_ref, swapped_ref, one_ref, two_ref, here_ref, three_ref, six_ref):
    pair = here_ref.shape[0]
    share = pair // 2
    here_ref[...] = (
        kept_ref[:pair, :] + one_ref[:pair, :].astype(F32) + two_ref[:pair, :].astype(F32)
    )
    three_ref[...] = (
        kept_ref[pair : 2 * pair, :]
        + swapped_ref[:pair, :].astype(F32)
        + one_ref[pair : 2 * pair, :].astype(F32)
        + two_ref[pair : 2 * pair, :].astype(F32)
    ).astype(BF16)
    sixth = (
        kept_ref[2 * pair : 3 * pair, :]
        + swapped_ref[pair : 2 * pair, :].astype(F32)
        + one_ref[2 * pair :, :].astype(F32)
    )
    own = sixth[:share, :] + two_ref[2 * pair :, :].astype(F32)
    six_ref[:share, :] = own.astype(BF16)
    six_ref[share:, :] = sixth[share:, :].astype(BF16)


def last_kernel(here_ref, three_ref, six_ref, own_ref, partner_ref):
    share = own_ref.shape[0]
    total = here_ref[...] + three_ref[...].astype(F32) + six_ref[...].astype(F32)
    own_ref[...] = total[:share, :]
    partner_ref[...] = total[share:, :].astype(BF16)


def summed_line(kept, swapped, share):
    width = kept.shape[1]
    pair = 2 * share
    one, two = pl.pallas_call(
        near_kernel,
        out_shape=(shape(3 * pair, width, BF16), shape(2 * pair + share, width, BF16)),
    )(kept, swapped)
    one = along(one, NEAR[0])
    two = along(two, NEAR[1])
    here, three, six = pl.pallas_call(
        far_kernel,
        out_shape=(shape(pair, width, F32), shape(pair, width, BF16), shape(pair, width, BF16)),
    )(kept, swapped, one, two)
    three = along(three, FAR[0])
    six = along(six, FAR[1])
    own, partner = pl.pallas_call(
        last_kernel, out_shape=(shape(share, width, F32), shape(share, width, BF16))
    )(here, three, six)
    partner = exchange(partner, "c", 1)
    return own + partner.astype(F32)


LANES = 128
SUM_ROWS = 16


def pack_kernel(back_ref, sums_ref, text_ref, out_ref):
    heads = out_ref.shape[0]
    cols = back_ref.shape[0] // heads
    half = cols // 2
    side = LANES // 2
    share, width = text_ref.shape
    for h in range(heads):
        block = back_ref[h * cols : (h + 1) * cols, :]
        out_ref[h, :cols, :] = block[:, :LANES]
        out_ref[h, cols : cols + half, :side] = block[:half, LANES:]
        out_ref[h, cols : cols + half, side:] = block[half:, LANES:]
        out_ref[h, cols + half : cols + half + SUM_ROWS, :] = sums_ref[...]
        for k in range(width // LANES):
            first = cols + half + SUM_ROWS + k * share
            out_ref[h, first : first + share, :] = text_ref[:, k * LANES : (k + 1) * LANES]


def finish_kernel(
    packed_ref, direct_ref, centred_ref, inv_ref, gain_ref, mapping_ref, image_ref, text_ref, rows_ref
):
    heads = packed_ref.shape[0]
    cols, rows = direct_ref.shape
    half = cols // 2
    side = LANES // 2
    width = mapping_ref.shape[1]
    share = rows // heads
    tail = cols + half + SUM_ROWS

    def added(first, last):
        total = packed_ref[0, first:last, :].astype(F32)
        for h in range(1, heads):
            total = total + packed_ref[h, first:last, :].astype(F32)
        return total

    sums = added(cols + half, tail)
    low = added(0, cols)
    high = added(cols, cols + half)

    def store(top, bottom, here, part, row):
        span = part.shape[1]
        one = (sums[row : row + 1, :span] + sums[row + 4 : row + 5, :span]) / width
        two = (sums[row + 2 : row + 3, :span] + sums[row + 6 : row + 7, :span]) / width
        image_ref[top:bottom, here] = direct_ref[top:bottom, here] + inv_ref[:, here] * (
            part * gain_ref[top:bottom, :] - one - centred_ref[top:bottom, here] * two
        )

    store(0, cols, slice(0, LANES), low, 0)
    store(0, half, slice(LANES, rows), high[:, :side], 1)
    store(half, cols, slice(LANES, rows), high[:, side:], 1)
    for h in range(heads):
        for k in range(width // LANES):
            first = tail + k * share
            rows_ref[h * share : (h + 1) * share, k * LANES : (k + 1) * LANES] = packed_ref[
                h, first : first + share, :
            ]
    text_ref[...] = dot(mapping_ref[...], rows_ref[...], ((1,), (1,)))


def gelu_tanh(values):
    return jax.nn.gelu(values, approximate=True)


def norm_back(upstream, unit_rows, inverse):
    unit_float = unit_rows.astype(F32)
    along = jnp.sum(unit_float * upstream, axis=-1, keepdims=True)
    return inverse * (upstream - unit_float * along)


def dot(a, b, dims):
    return lax.dot_general(a, b, (dims, ((), ())), preferred_element_type=F32)


def per_device(picture, caption, gain, entry, exit_matrix, mapping, scale, offset):
    rows = picture.shape[0]
    width = picture.shape[1]
    heads = lax.axis_size(MP)
    head_pos = lax.axis_index(MP)
    share = rows // heads
    cols = caption.shape[1]
    first_row = head_pos * share
    first_col = head_pos * cols
    text_part = dot(caption, mapping, ((1,), (0,))).astype(BF16)
    image_float = picture.astype(F32)
    mean_row = jnp.mean(image_float, axis=-1, keepdims=True)
    variance = jnp.mean((image_float - mean_row) ** 2, axis=-1, keepdims=True)
    inv_std = lax.rsqrt(variance + 1e-06)
    centred = (image_float - mean_row) * inv_std
    normed = (centred * gain).astype(BF16)
    preact = dot(normed, entry, ((1,), (0,)))
    entry_gain = jnp.sum(entry.astype(F32) * gain[:, None], axis=0)
    hidden = gelu_tanh(preact).astype(BF16)
    partial_out = dot(hidden, exit_matrix, ((1,), (0,))).astype(BF16)
    own_rows = lax.dynamic_slice_in_dim(picture, first_row, share, 0).astype(F32)
    parts = [p.reshape(heads, share, width) for p in (text_part, partial_out)]
    sums = jnp.sum(swap(jnp.concatenate(parts, axis=1), MP).astype(F32), axis=0)
    text_out = sums[:share]
    inv_text = lax.rsqrt(jnp.sum(text_out * text_out, axis=-1, keepdims=True) + 1e-06)
    unit_text = (text_out * inv_text).astype(BF16)
    image_out = own_rows + sums[share:]
    inv_image = lax.rsqrt(jnp.sum(image_out * image_out, axis=-1, keepdims=True) + 1e-06)
    unit_image = (image_out * inv_image).astype(BF16)

    pieces = gathered_line(unit_text)
    images = spread(unit_image, XY)

    own_start = (lax.axis_index(XY) * share).reshape(1)
    consts = jnp.stack([scale, offset])
    sent_rows = pieces[-1].shape[0]
    kept_rows = sum(p.shape[0] for p in pieces) - sent_rows
    scalars = pl.BlockSpec(memory_space=pltpu.SMEM)
    whole = pl.BlockSpec(memory_space=pltpu.VMEM)
    text_sent, text_kept, image_add = pl.pallas_call(
        functools.partial(pairs_kernel, share),
        in_specs=[scalars, scalars] + [whole] * 7,
        out_shape=(
            shape(sent_rows, width, BF16),
            shape(kept_rows, width, F32),
            shape(images.shape[0], width, BF16),
        ),
        scratch_shapes=[
            pltpu.VMEM((sent_rows + kept_rows, width), BF16),
            pltpu.VMEM((sent_rows + kept_rows, images.shape[0]), BF16),
        ],
    )(consts, own_start, *pieces, images)

    image_parts = swap(image_add.reshape(-1, share, width), XY)
    image_dir = jnp.sum(image_parts.astype(F32), axis=0)
    grad_share = norm_back(image_dir, unit_image, inv_image).astype(BF16)
    grad_out_b = spread(grad_share, MP)

    swapped = exchange(text_sent, "c", 1)
    text_dir = summed_line(text_kept, swapped, share)
    grad_text_share = norm_back(text_dir, unit_text, inv_text).astype(BF16)

    grad_hidden = dot(grad_out_b, exit_matrix, ((1,), (1,)))
    unused, pull_back = jax.vjp(gelu_tanh, preact)
    grad_pre = pull_back(grad_hidden)[0].astype(BF16)
    back = dot(entry, grad_pre, ((1,), (1,))).astype(BF16)
    pre_float = grad_pre.astype(F32)
    row_sums = jnp.stack(
        [jnp.sum(pre_float * entry_gain, axis=-1), jnp.sum(pre_float * preact, axis=-1)]
    )
    sums_high = lax.reduce_precision(row_sums, 8, 7)
    sums_low = row_sums - sums_high
    sums_both = jnp.concatenate([sums_high, sums_low], axis=0).astype(BF16)
    sums_both = jnp.pad(sums_both, ((0, 0), (0, 2 * LANES - rows))).reshape(-1, LANES)
    sums_both = jnp.pad(sums_both, ((0, SUM_ROWS - sums_both.shape[0]), (0, 0)))
    length = cols + cols // 2 + SUM_ROWS + share * width // LANES
    packed = pl.pallas_call(
        pack_kernel, out_shape=jax.ShapeDtypeStruct((heads, length, LANES), BF16)
    )(back, sums_both, grad_text_share)
    arrived = swap(packed, MP)
    gain_here = lax.dynamic_slice_in_dim(gain, first_col, cols, 0)
    feature = jnp.arange(width, dtype=jnp.int32)[None, :] - first_col
    chosen = (feature == jnp.arange(cols, dtype=jnp.int32)[:, None]).astype(BF16)
    picture_here = dot(chosen, picture, ((1,), (1,)))
    centred_here = (picture_here - mean_row.T) * inv_std.T
    direct = dot(chosen, grad_out_b, ((1,), (1,)))
    outs = jax.ShapeDtypeStruct((cols, rows), F32)
    grad_image, grad_text, unused = pl.pallas_call(
        finish_kernel, out_shape=(outs, outs, jax.ShapeDtypeStruct((rows, width), BF16))
    )(arrived, direct, centred_here, inv_std.T, gain_here[:, None], mapping)
    return (grad_image.T, grad_text.T)


def solution(mesh):
    split = Mesh(mesh.devices.reshape(4, 4, 2, 2, 4, 2), (*DP, *MP))
    in_specs = (
        P(DP, None),
        P(DP, MP),
        P(),
        P(None, MP),
        P(MP, None),
        P(MP, None),
        P(),
        P(),
    )
    out_specs = (P(DP, MP), P(DP, MP))
    return jax.shard_map(
        per_device, mesh=split, in_specs=in_specs, out_specs=out_specs, check_vma=False
    )
```

```python
import functools

import jax
import jax.numpy as jnp
from jax import lax
from jax.experimental import pallas as pl
from jax.experimental.pallas import tpu as pltpu
from jax.sharding import Mesh
from jax.sharding import PartitionSpec as P


DP = ("zh", "zl", "yl", "c")
MP = ("x", "yh")
Z = ("zh", "zl")
XY = ("yl", "x", "yh")
LINE = ("zh", "zl", "c")
NEAR = (1, 2)
FAR = (3, 6)
F32 = jnp.float32
BF16 = jnp.bfloat16


def swap(array, axes):
    return lax.all_to_all(array, axes, 0, 0, tiled=True)


def exchange(array, axes, k):
    n = lax.axis_size(axes)
    return lax.ppermute(array, axes, [(i, i ^ k) for i in range(n)])


def spread(array, axes):
    n = lax.axis_size(axes)
    copies = jnp.broadcast_to(array[None], (n, *array.shape))
    return swap(copies, axes).reshape(n * array.shape[0], *array.shape[1:])


def along(array, k):
    n = lax.axis_size(Z)
    moves = []
    for i in range(n):
        moves.append((2 * i, 2 * ((i - k) % n)))
        moves.append((2 * i + 1, 2 * ((i + k) % n) + 1))
    return lax.ppermute(array, LINE, moves)


def gathered_line(array):
    share = array.shape[0]
    pair = jnp.concatenate([array, exchange(array, "c", 1)], axis=0)
    third = along(pair, -FAR[0])
    far = [third, along(third, FAR[0] - FAR[1])]
    near = jnp.concatenate([pair, *far], axis=0)
    cut = near.shape[0] - share
    last = [along(near, -NEAR[0]), along(near[:cut], -NEAR[1])]
    other = exchange(jnp.concatenate([*far, *last], axis=0), "c", 1)
    return [pair, *far, *last, other]


def shape(rows, width, dtype):
    return jax.ShapeDtypeStruct((rows, width), dtype)


def pairs_kernel(share, consts_ref, start_ref, *refs):
    pieces, images_ref = refs[:6], refs[6]
    sent_ref, kept_ref, image_ref, texts_ref, weights_ref = refs[7:]
    at = 0
    for piece in pieces:
        texts_ref[at : at + piece.shape[0], :] = piece[...]
        at += piece.shape[0]
    scale = consts_ref[0]
    step = at // 6
    columns = images_ref.shape[0]
    for first in range(0, at, step):
        energies = scale * dot(
            texts_ref[first : first + step, :], images_ref[...], ((1,), (1,))
        ) + consts_ref[1]
        if first:
            weights = scale * jax.nn.sigmoid(energies)
        else:
            text_ids = lax.broadcasted_iota(jnp.int32, (step, columns), 0)
            image_ids = lax.broadcasted_iota(jnp.int32, (step, columns), 1) - start_ref[0]
            same = (text_ids == image_ids) & (text_ids < share)
            polarity = jnp.where(same, 1.0, -1.0).astype(F32)
            weights = scale * -polarity * jax.nn.sigmoid(-polarity * energies)
        weights_ref[first : first + step, :] = weights.astype(BF16)
    middle = kept_ref.shape[0]
    sent_ref[...] = dot(weights_ref[middle:, :], images_ref[...], ((1,), (0,))).astype(BF16)
    kept_ref[...] = dot(weights_ref[:middle, :], images_ref[...], ((1,), (0,))).astype(BF16)
    image_ref[...] = dot(weights_ref[...], texts_ref[...], ((0,), (0,))).astype(BF16)


def near_kernel(kept_ref, swapped_ref, one_ref, two_ref):
    long = one_ref.shape[0]
    pair = long // 3
    one_ref[...] = (
        kept_ref[3 * pair : 6 * pair, :].astype(F32)
        + swapped_ref[2 * pair : 5 * pair, :].astype(F32)
    ).astype(BF16)
    two_ref[...] = (
        kept_ref[6 * pair :, :].astype(F32) + swapped_ref[5 * pair :, :].astype(F32)
    ).astype(BF16)


def far_kernel(kept_ref, swapped_ref, one_ref, two_ref, here_ref, three_ref, six_ref):
    pair = here_ref.shape[0]
    share = pair // 2
    here_ref[...] = (
        kept_ref[:pair, :].astype(F32)
        + one_ref[:pair, :].astype(F32)
        + two_ref[:pair, :].astype(F32)
    )
    three_ref[...] = (
        kept_ref[pair : 2 * pair, :].astype(F32)
        + swapped_ref[:pair, :].astype(F32)
        + one_ref[pair : 2 * pair, :].astype(F32)
        + two_ref[pair : 2 * pair, :].astype(F32)
    ).astype(BF16)
    sixth = (
        kept_ref[2 * pair : 3 * pair, :].astype(F32)
        + swapped_ref[pair : 2 * pair, :].astype(F32)
        + one_ref[2 * pair :, :].astype(F32)
    )
    own = sixth[:share, :] + two_ref[2 * pair :, :].astype(F32)
    six_ref[:share, :] = own.astype(BF16)
    six_ref[share:, :] = sixth[share:, :].astype(BF16)


def last_kernel(here_ref, three_ref, six_ref, own_ref, partner_ref):
    share = own_ref.shape[0]
    total = here_ref[...] + three_ref[...].astype(F32) + six_ref[...].astype(F32)
    own_ref[...] = total[:share, :]
    partner_ref[...] = total[share:, :].astype(BF16)


def summed_line(kept, swapped, share):
    width = kept.shape[1]
    pair = 2 * share
    one, two = pl.pallas_call(
        near_kernel,
        out_shape=(shape(3 * pair, width, BF16), shape(2 * pair + share, width, BF16)),
    )(kept, swapped)
    one = along(one, NEAR[0])
    two = along(two, NEAR[1])
    here, three, six = pl.pallas_call(
        far_kernel,
        out_shape=(shape(pair, width, F32), shape(pair, width, BF16), shape(pair, width, BF16)),
    )(kept, swapped, one, two)
    three = along(three, FAR[0])
    six = along(six, FAR[1])
    own, partner = pl.pallas_call(
        last_kernel, out_shape=(shape(share, width, F32), shape(share, width, BF16))
    )(here, three, six)
    partner = exchange(partner, "c", 1)
    return own + partner.astype(F32)


LANES = 128
SUM_ROWS = 16


def pack_kernel(back_ref, sums_ref, text_ref, out_ref):
    heads = out_ref.shape[0]
    cols = back_ref.shape[0] // heads
    half = cols // 2
    side = LANES // 2
    share, width = text_ref.shape
    for h in range(heads):
        block = back_ref[h * cols : (h + 1) * cols, :]
        out_ref[h, :cols, :] = block[:, :LANES]
        out_ref[h, cols : cols + half, :side] = block[:half, LANES:]
        out_ref[h, cols : cols + half, side:] = block[half:, LANES:]
        out_ref[h, cols + half : cols + half + SUM_ROWS, :] = sums_ref[...]
        for k in range(width // LANES):
            first = cols + half + SUM_ROWS + k * share
            out_ref[h, first : first + share, :] = text_ref[:, k * LANES : (k + 1) * LANES]


def finish_kernel(
    packed_ref, direct_ref, centred_ref, inv_ref, gain_ref, mapping_ref, image_ref, text_ref, rows_ref
):
    heads = packed_ref.shape[0]
    cols, rows = direct_ref.shape
    half = cols // 2
    side = LANES // 2
    width = mapping_ref.shape[1]
    share = rows // heads
    tail = cols + half + SUM_ROWS

    def added(first, last):
        total = packed_ref[0, first:last, :].astype(F32)
        for h in range(1, heads):
            total = total + packed_ref[h, first:last, :].astype(F32)
        return total

    sums = added(cols + half, tail)
    low = added(0, cols)
    high = added(cols, cols + half)

    def store(top, bottom, here, part, row):
        span = part.shape[1]
        one = (sums[row : row + 1, :span] + sums[row + 4 : row + 5, :span]) / width
        two = (sums[row + 2 : row + 3, :span] + sums[row + 6 : row + 7, :span]) / width
        image_ref[top:bottom, here] = direct_ref[top:bottom, here] + inv_ref[:, here] * (
            part * gain_ref[top:bottom, :] - one - centred_ref[top:bottom, here] * two
        )

    store(0, cols, slice(0, LANES), low, 0)
    store(0, half, slice(LANES, rows), high[:, :side], 1)
    store(half, cols, slice(LANES, rows), high[:, side:], 1)
    for h in range(heads):
        for k in range(width // LANES):
            first = tail + k * share
            rows_ref[h * share : (h + 1) * share, k * LANES : (k + 1) * LANES] = packed_ref[
                h, first : first + share, :
            ]
    text_ref[...] = dot(mapping_ref[...], rows_ref[...], ((1,), (1,)))


def gelu_tanh(values):
    return jax.nn.gelu(values, approximate=True)


def norm_back(upstream, unit_rows, inverse):
    unit_float = unit_rows.astype(F32)
    along = jnp.sum(unit_float * upstream, axis=-1, keepdims=True)
    return inverse * (upstream - unit_float * along)


def dot(a, b, dims):
    return lax.dot_general(a, b, (dims, ((), ())), preferred_element_type=F32)


def per_device(picture, caption, gain, entry, exit_matrix, mapping, scale, offset):
    rows = picture.shape[0]
    width = picture.shape[1]
    heads = lax.axis_size(MP)
    head_pos = lax.axis_index(MP)
    share = rows // heads
    cols = caption.shape[1]
    first_row = head_pos * share
    first_col = head_pos * cols
    text_part = dot(caption, mapping, ((1,), (0,))).astype(BF16)
    image_float = picture.astype(F32)
    mean_row = jnp.mean(image_float, axis=-1, keepdims=True)
    variance = jnp.mean((image_float - mean_row) ** 2, axis=-1, keepdims=True)
    inv_std = lax.rsqrt(variance + 1e-06)
    centred = (image_float - mean_row) * inv_std
    normed = (centred * gain).astype(BF16)
    preact = dot(normed, entry, ((1,), (0,)))
    entry_gain = jnp.sum(entry.astype(F32) * gain[:, None], axis=0)
    hidden = gelu_tanh(preact).astype(BF16)
    partial_out = dot(hidden, exit_matrix, ((1,), (0,))).astype(BF16)
    own_rows = lax.dynamic_slice_in_dim(picture, first_row, share, 0).astype(F32)
    parts = [p.reshape(heads, share, width) for p in (text_part, partial_out)]
    sums = jnp.sum(swap(jnp.concatenate(parts, axis=1), MP).astype(F32), axis=0)
    text_out = sums[:share]
    inv_text = lax.rsqrt(jnp.sum(text_out * text_out, axis=-1, keepdims=True) + 1e-06)
    unit_text = (text_out * inv_text).astype(BF16)
    image_out = own_rows + sums[share:]
    inv_image = lax.rsqrt(jnp.sum(image_out * image_out, axis=-1, keepdims=True) + 1e-06)
    unit_image = (image_out * inv_image).astype(BF16)

    pieces = gathered_line(unit_text)
    images = spread(unit_image, XY)

    own_start = (lax.axis_index(XY) * share).reshape(1)
    consts = jnp.stack([scale, offset])
    sent_rows = pieces[-1].shape[0]
    kept_rows = sum(p.shape[0] for p in pieces) - sent_rows
    scalars = pl.BlockSpec(memory_space=pltpu.SMEM)
    whole = pl.BlockSpec(memory_space=pltpu.VMEM)
    text_sent, text_kept, image_add = pl.pallas_call(
        functools.partial(pairs_kernel, share),
        in_specs=[scalars, scalars] + [whole] * 7,
        out_shape=(
            shape(sent_rows, width, BF16),
            shape(kept_rows, width, BF16),
            shape(images.shape[0], width, BF16),
        ),
        scratch_shapes=[
            pltpu.VMEM((sent_rows + kept_rows, width), BF16),
            pltpu.VMEM((sent_rows + kept_rows, images.shape[0]), BF16),
        ],
    )(consts, own_start, *pieces, images)

    image_parts = swap(image_add.reshape(-1, share, width), XY)
    image_dir = jnp.sum(image_parts.astype(F32), axis=0)
    grad_share = norm_back(image_dir, unit_image, inv_image).astype(BF16)
    grad_out_b = spread(grad_share, MP)

    swapped = exchange(text_sent, "c", 1)
    text_dir = summed_line(text_kept, swapped, share)
    grad_text_share = norm_back(text_dir, unit_text, inv_text).astype(BF16)

    grad_hidden = dot(grad_out_b, exit_matrix, ((1,), (1,)))
    unused, pull_back = jax.vjp(gelu_tanh, preact)
    grad_pre = pull_back(grad_hidden)[0].astype(BF16)
    back = dot(entry, grad_pre, ((1,), (1,))).astype(BF16)
    pre_float = grad_pre.astype(F32)
    row_sums = jnp.stack(
        [jnp.sum(pre_float * entry_gain, axis=-1), jnp.sum(pre_float * preact, axis=-1)]
    )
    sums_high = lax.reduce_precision(row_sums, 8, 7)
    sums_low = row_sums - sums_high
    sums_both = jnp.concatenate([sums_high, sums_low], axis=0).astype(BF16)
    sums_both = jnp.pad(sums_both, ((0, 0), (0, 2 * LANES - rows))).reshape(-1, LANES)
    sums_both = jnp.pad(sums_both, ((0, SUM_ROWS - sums_both.shape[0]), (0, 0)))
    length = cols + cols // 2 + SUM_ROWS + share * width // LANES
    packed = pl.pallas_call(
        pack_kernel, out_shape=jax.ShapeDtypeStruct((heads, length, LANES), BF16)
    )(back, sums_both, grad_text_share)
    arrived = swap(packed, MP)
    gain_here = lax.dynamic_slice_in_dim(gain, first_col, cols, 0)
    feature = jnp.arange(width, dtype=jnp.int32)[None, :] - first_col
    chosen = (feature == jnp.arange(cols, dtype=jnp.int32)[:, None]).astype(BF16)
    picture_here = dot(chosen, picture, ((1,), (1,)))
    centred_here = (picture_here - mean_row.T) * inv_std.T
    direct = dot(chosen, grad_out_b, ((1,), (1,)))
    outs = jax.ShapeDtypeStruct((cols, rows), F32)
    grad_image, grad_text, unused = pl.pallas_call(
        finish_kernel, out_shape=(outs, outs, jax.ShapeDtypeStruct((rows, width), BF16))
    )(arrived, direct, centred_here, inv_std.T, gain_here[:, None], mapping)
    return (grad_image.T, grad_text.T)


def solution(mesh):
    split = Mesh(mesh.devices.reshape(4, 4, 2, 2, 4, 2), (*DP, *MP))
    in_specs = (
        P(DP, None),
        P(DP, MP),
        P(),
        P(None, MP),
        P(MP, None),
        P(MP, None),
        P(),
        P(),
    )
    out_specs = (P(DP, MP), P(DP, MP))
    return jax.shard_map(
        per_device, mesh=split, in_specs=in_specs, out_specs=out_specs, check_vma=False
    )
```

```python
import functools

import jax
import jax.numpy as jnp
from jax import lax
from jax.experimental import pallas as pl
from jax.experimental.pallas import tpu as pltpu
from jax.sharding import Mesh
from jax.sharding import PartitionSpec as P


DP = ("zh", "zl", "yl", "c")
MP = ("x", "yh")
Z = ("zh", "zl")
XY = ("yl", "x", "yh")
LINE = ("zh", "zl", "c")
NEAR = (1, 2)
FAR = (3, 6)
F32 = jnp.float32
BF16 = jnp.bfloat16


def swap(array, axes):
    return lax.all_to_all(array, axes, 0, 0, tiled=True)


def exchange(array, axes, k):
    n = lax.axis_size(axes)
    return lax.ppermute(array, axes, [(i, i ^ k) for i in range(n)])


def spread(array, axes):
    n = lax.axis_size(axes)
    copies = jnp.broadcast_to(array[None], (n, *array.shape))
    return swap(copies, axes).reshape(n * array.shape[0], *array.shape[1:])


def along(array, k):
    n = lax.axis_size(Z)
    moves = []
    for i in range(n):
        moves.append((2 * i, 2 * ((i - k) % n)))
        moves.append((2 * i + 1, 2 * ((i + k) % n) + 1))
    return lax.ppermute(array, LINE, moves)


def gathered_line(array):
    share = array.shape[0]
    pair = jnp.concatenate([array, exchange(array, "c", 1)], axis=0)
    third = along(pair, -FAR[0])
    far = [third, along(third, FAR[0] - FAR[1])]
    near = jnp.concatenate([pair, *far], axis=0)
    cut = near.shape[0] - share
    last = [along(near, -NEAR[0]), along(near[:cut], -NEAR[1])]
    other = exchange(jnp.concatenate([*far, *last], axis=0), "c", 1)
    return [pair, *far, *last, other]


LIMIT = pltpu.CompilerParams(vmem_limit_bytes=32 << 20)


def near_core(array):
    return pltpu.with_memory_space_constraint(array, pltpu.VMEM)


def in_fast_memory(kernel, out_shape):
    kept = jax.tree.map(lambda s: pltpu.VMEM(s.shape, s.dtype), out_shape)
    run = pl.pallas_call(kernel, out_shape=kept, compiler_params=LIMIT)
    return lambda *operands: run(*(near_core(x) for x in operands))


def shape(rows, width, dtype):
    return jax.ShapeDtypeStruct((rows, width), dtype)


def pairs_kernel(share, consts_ref, start_ref, *refs):
    pieces, images_ref = refs[:6], refs[6]
    sent_ref, kept_ref, image_ref, texts_ref, weights_ref = refs[7:]
    at = 0
    for piece in pieces:
        texts_ref[at : at + piece.shape[0], :] = piece[...]
        at += piece.shape[0]
    scale = consts_ref[0]
    step = at // 6
    columns = images_ref.shape[0]
    for first in range(0, at, step):
        energies = scale * dot(
            texts_ref[first : first + step, :], images_ref[...], ((1,), (1,))
        ) + consts_ref[1]
        if first:
            weights = scale * jax.nn.sigmoid(energies)
        else:
            text_ids = lax.broadcasted_iota(jnp.int32, (step, columns), 0)
            image_ids = lax.broadcasted_iota(jnp.int32, (step, columns), 1) - start_ref[0]
            same = (text_ids == image_ids) & (text_ids < share)
            polarity = jnp.where(same, 1.0, -1.0).astype(F32)
            weights = scale * -polarity * jax.nn.sigmoid(-polarity * energies)
        weights_ref[first : first + step, :] = weights.astype(BF16)
    middle = kept_ref.shape[0]
    sent_ref[...] = dot(weights_ref[middle:, :], images_ref[...], ((1,), (0,))).astype(BF16)
    kept_ref[...] = dot(weights_ref[:middle, :], images_ref[...], ((1,), (0,))).astype(BF16)
    image_ref[...] = dot(weights_ref[...], texts_ref[...], ((0,), (0,))).astype(BF16)


def near_kernel(kept_ref, swapped_ref, one_ref, two_ref):
    long = one_ref.shape[0]
    pair = long // 3
    one_ref[...] = (
        kept_ref[3 * pair : 6 * pair, :].astype(F32)
        + swapped_ref[2 * pair : 5 * pair, :].astype(F32)
    ).astype(BF16)
    two_ref[...] = (
        kept_ref[6 * pair :, :].astype(F32) + swapped_ref[5 * pair :, :].astype(F32)
    ).astype(BF16)


def far_kernel(kept_ref, swapped_ref, one_ref, two_ref, here_ref, three_ref, six_ref):
    pair = here_ref.shape[0]
    share = pair // 2
    here_ref[...] = (
        kept_ref[:pair, :].astype(F32)
        + one_ref[:pair, :].astype(F32)
        + two_ref[:pair, :].astype(F32)
    )
    three_ref[...] = (
        kept_ref[pair : 2 * pair, :].astype(F32)
        + swapped_ref[:pair, :].astype(F32)
        + one_ref[pair : 2 * pair, :].astype(F32)
        + two_ref[pair : 2 * pair, :].astype(F32)
    ).astype(BF16)
    sixth = (
        kept_ref[2 * pair : 3 * pair, :].astype(F32)
        + swapped_ref[pair : 2 * pair, :].astype(F32)
        + one_ref[2 * pair :, :].astype(F32)
    )
    own = sixth[:share, :] + two_ref[2 * pair :, :].astype(F32)
    six_ref[:share, :] = own.astype(BF16)
    six_ref[share:, :] = sixth[share:, :].astype(BF16)


def last_kernel(here_ref, three_ref, six_ref, own_ref, partner_ref):
    share = own_ref.shape[0]
    total = here_ref[...] + three_ref[...].astype(F32) + six_ref[...].astype(F32)
    own_ref[...] = total[:share, :]
    partner_ref[...] = total[share:, :].astype(BF16)


def summed_line(kept, swapped, share):
    width = kept.shape[1]
    pair = 2 * share
    one, two = in_fast_memory(
        near_kernel,
        (shape(3 * pair, width, BF16), shape(2 * pair + share, width, BF16)),
    )(kept, swapped)
    one = along(one, NEAR[0])
    two = along(two, NEAR[1])
    here, three, six = in_fast_memory(
        far_kernel,
        (shape(pair, width, F32), shape(pair, width, BF16), shape(pair, width, BF16)),
    )(kept, swapped, one, two)
    three = along(three, FAR[0])
    six = along(six, FAR[1])
    own, partner = in_fast_memory(
        last_kernel, (shape(share, width, F32), shape(share, width, BF16))
    )(here, three, six)
    partner = exchange(partner, "c", 1)
    return own + partner.astype(F32)


LANES = 128
SUM_ROWS = 16


def pack_kernel(back_ref, sums_ref, text_ref, out_ref):
    heads = out_ref.shape[0]
    cols = back_ref.shape[0] // heads
    half = cols // 2
    side = LANES // 2
    share, width = text_ref.shape
    for h in range(heads):
        block = back_ref[h * cols : (h + 1) * cols, :]
        out_ref[h, :cols, :] = block[:, :LANES]
        out_ref[h, cols : cols + half, :side] = block[:half, LANES:]
        out_ref[h, cols : cols + half, side:] = block[half:, LANES:]
        out_ref[h, cols + half : cols + half + SUM_ROWS, :] = sums_ref[...]
        for k in range(width // LANES):
            first = cols + half + SUM_ROWS + k * share
            out_ref[h, first : first + share, :] = text_ref[:, k * LANES : (k + 1) * LANES]


def finish_kernel(
    packed_ref, direct_ref, centred_ref, inv_ref, gain_ref, mapping_ref, image_ref, text_ref, rows_ref
):
    heads = packed_ref.shape[0]
    cols, rows = direct_ref.shape
    half = cols // 2
    side = LANES // 2
    width = mapping_ref.shape[1]
    share = rows // heads
    tail = cols + half + SUM_ROWS

    def added(first, last):
        total = packed_ref[0, first:last, :].astype(F32)
        for h in range(1, heads):
            total = total + packed_ref[h, first:last, :].astype(F32)
        return total

    sums = added(cols + half, tail)
    low = added(0, cols)
    high = added(cols, cols + half)

    def store(top, bottom, here, part, row):
        span = part.shape[1]
        one = (sums[row : row + 1, :span] + sums[row + 4 : row + 5, :span]) / width
        two = (sums[row + 2 : row + 3, :span] + sums[row + 6 : row + 7, :span]) / width
        image_ref[top:bottom, here] = direct_ref[top:bottom, here] + inv_ref[:, here] * (
            part * gain_ref[top:bottom, :] - one - centred_ref[top:bottom, here] * two
        )

    store(0, cols, slice(0, LANES), low, 0)
    store(0, half, slice(LANES, rows), high[:, :side], 1)
    store(half, cols, slice(LANES, rows), high[:, side:], 1)
    for h in range(heads):
        for k in range(width // LANES):
            first = tail + k * share
            rows_ref[h * share : (h + 1) * share, k * LANES : (k + 1) * LANES] = packed_ref[
                h, first : first + share, :
            ]
    text_ref[...] = dot(mapping_ref[...], rows_ref[...], ((1,), (1,)))


def gelu_tanh(values):
    return jax.nn.gelu(values, approximate=True)


def norm_back(upstream, unit_rows, inverse):
    unit_float = unit_rows.astype(F32)
    along = jnp.sum(unit_float * upstream, axis=-1, keepdims=True)
    return inverse * (upstream - unit_float * along)


def dot(a, b, dims):
    return lax.dot_general(a, b, (dims, ((), ())), preferred_element_type=F32)


def per_device(picture, caption, gain, entry, exit_matrix, mapping, scale, offset):
    rows = picture.shape[0]
    width = picture.shape[1]
    heads = lax.axis_size(MP)
    head_pos = lax.axis_index(MP)
    share = rows // heads
    cols = caption.shape[1]
    first_row = head_pos * share
    first_col = head_pos * cols
    text_part = dot(caption, mapping, ((1,), (0,))).astype(BF16)
    image_float = picture.astype(F32)
    mean_row = jnp.mean(image_float, axis=-1, keepdims=True)
    variance = jnp.mean((image_float - mean_row) ** 2, axis=-1, keepdims=True)
    inv_std = lax.rsqrt(variance + 1e-06)
    centred = (image_float - mean_row) * inv_std
    normed = (centred * gain).astype(BF16)
    preact = dot(normed, entry, ((1,), (0,)))
    entry_gain = jnp.sum(entry.astype(F32) * gain[:, None], axis=0)
    hidden = gelu_tanh(preact).astype(BF16)
    partial_out = dot(hidden, exit_matrix, ((1,), (0,))).astype(BF16)
    own_rows = lax.dynamic_slice_in_dim(picture, first_row, share, 0).astype(F32)
    parts = [p.reshape(heads, share, width) for p in (text_part, partial_out)]
    sums = jnp.sum(swap(jnp.concatenate(parts, axis=1), MP).astype(F32), axis=0)
    text_out = sums[:share]
    inv_text = lax.rsqrt(jnp.sum(text_out * text_out, axis=-1, keepdims=True) + 1e-06)
    unit_text = (text_out * inv_text).astype(BF16)
    image_out = own_rows + sums[share:]
    inv_image = lax.rsqrt(jnp.sum(image_out * image_out, axis=-1, keepdims=True) + 1e-06)
    unit_image = (image_out * inv_image).astype(BF16)

    pieces = gathered_line(unit_text)
    images = spread(unit_image, XY)

    own_start = (lax.axis_index(XY) * share).reshape(1)
    consts = jnp.stack([scale, offset])
    sent_rows = pieces[-1].shape[0]
    kept_rows = sum(p.shape[0] for p in pieces) - sent_rows
    scalars = pl.BlockSpec(memory_space=pltpu.SMEM)
    whole = pl.BlockSpec(memory_space=pltpu.VMEM)
    text_sent, text_kept, image_add = pl.pallas_call(
        functools.partial(pairs_kernel, share),
        in_specs=[scalars, scalars] + [whole] * 7,
        out_specs=(whole, whole, whole),
        out_shape=(
            pltpu.VMEM((sent_rows, width), BF16),
            pltpu.VMEM((kept_rows, width), BF16),
            pltpu.VMEM((images.shape[0], width), BF16),
        ),
        compiler_params=LIMIT,
        scratch_shapes=[
            pltpu.VMEM((sent_rows + kept_rows, width), BF16),
            pltpu.VMEM((sent_rows + kept_rows, images.shape[0]), BF16),
        ],
    )(consts, own_start, *(near_core(x) for x in (*pieces, images)))

    image_parts = swap(image_add.reshape(-1, share, width), XY)
    image_dir = jnp.sum(image_parts.astype(F32), axis=0)
    grad_share = norm_back(image_dir, unit_image, inv_image).astype(BF16)
    grad_out_b = spread(grad_share, MP)

    swapped = exchange(text_sent, "c", 1)
    text_dir = summed_line(text_kept, swapped, share)
    grad_text_share = norm_back(text_dir, unit_text, inv_text).astype(BF16)

    grad_hidden = dot(grad_out_b, exit_matrix, ((1,), (1,)))
    unused, pull_back = jax.vjp(gelu_tanh, preact)
    grad_pre = pull_back(grad_hidden)[0].astype(BF16)
    back = dot(entry, grad_pre, ((1,), (1,))).astype(BF16)
    pre_float = grad_pre.astype(F32)
    row_sums = jnp.stack(
        [jnp.sum(pre_float * entry_gain, axis=-1), jnp.sum(pre_float * preact, axis=-1)]
    )
    sums_high = lax.reduce_precision(row_sums, 8, 7)
    sums_low = row_sums - sums_high
    sums_both = jnp.concatenate([sums_high, sums_low], axis=0).astype(BF16)
    sums_both = jnp.pad(sums_both, ((0, 0), (0, 2 * LANES - rows))).reshape(-1, LANES)
    sums_both = jnp.pad(sums_both, ((0, SUM_ROWS - sums_both.shape[0]), (0, 0)))
    length = cols + cols // 2 + SUM_ROWS + share * width // LANES
    packed = in_fast_memory(
        pack_kernel, jax.ShapeDtypeStruct((heads, length, LANES), BF16)
    )(back, sums_both, grad_text_share)
    arrived = swap(packed, MP)
    gain_here = lax.dynamic_slice_in_dim(gain, first_col, cols, 0)
    feature = jnp.arange(width, dtype=jnp.int32)[None, :] - first_col
    chosen = (feature == jnp.arange(cols, dtype=jnp.int32)[:, None]).astype(BF16)
    picture_here = dot(chosen, picture, ((1,), (1,)))
    centred_here = (picture_here - mean_row.T) * inv_std.T
    direct = dot(chosen, grad_out_b, ((1,), (1,)))
    outs = jax.ShapeDtypeStruct((cols, rows), F32)
    grad_image, grad_text, unused = pl.pallas_call(
        finish_kernel, out_shape=(outs, outs, jax.ShapeDtypeStruct((rows, width), BF16))
    )(arrived, direct, centred_here, inv_std.T, gain_here[:, None], mapping)
    return (grad_image.T, grad_text.T)


def solution(mesh):
    split = Mesh(mesh.devices.reshape(4, 4, 2, 2, 4, 2), (*DP, *MP))
    in_specs = (
        P(DP, None),
        P(DP, MP),
        P(),
        P(None, MP),
        P(MP, None),
        P(MP, None),
        P(),
        P(),
    )
    out_specs = (P(DP, MP), P(DP, MP))
    return jax.shard_map(
        per_device, mesh=split, in_specs=in_specs, out_specs=out_specs, check_vma=False
    )
```
